32 devices in a mesh: rows: 16 (over z, y, x), sub: 2 (over core).
Axes of the slice: x: 2, y: 2, z: 4, core: 2. Of those that a mesh axis runs over, the one named last changes fastest.
Arguments:
- matrix: float32 [4096, 384], P(('rows', 'sub')), as said below
- grad_out: float32 [4096, 384], P(('rows', 'sub')), as said below
- grad_factor: float32 [384, 384], replicated, may hold values from -6 to 6
Outputs:
- grad_matrix: float32 [4096, 384], P(('rows', 'sub'))
The draws below stay inside these ranges and needn't reach their ends.
Inputs may be any that keep to these rules, and one draw needn't show every extreme that they name: `matrix`: entries at most of order 1 / sqrt(4096), with a scale that varies by row and by column. `grad_out`: entries of order 0.01.
All inputs are finite; a program needn't handle non-finite values.
Results may differ from the reference program's by a relative error of at most 0.0004.
Values sent between devices are 32-bit elements; how exact they have to be, the bound alone decides.
No kernel may reach another device: no remote copies, remote signals or barrier semaphores. Data moves between devices by JAX's collectives and lax.ppermute only.
A program may use at most 64 MiB of HBM per device.

```python
import jax
import jax.numpy as jnp
from jax import lax

N = 384
SECTIONS = 2
R_DEV = 128
ROWS = 4096


def column_mix(key):
    gaussian = jax.random.normal(jax.random.fold_in(key, 15), (N, N), jnp.float32)
    rotation = jnp.linalg.qr(gaussian)[0]
    position = jnp.arange(N, dtype=jnp.float32) / (N - 1)
    column_decay = jnp.power(jnp.float32(10.0), -4.0 * jnp.cbrt(position))
    return column_decay[:, None] * rotation


def shared_rows(key):
    blocks = ROWS // R_DEV
    base_rows = jax.random.normal(jax.random.fold_in(key, 11), (ROWS, N), jnp.float32)
    block_scale = jnp.exp(jax.random.uniform(jax.random.fold_in(key, 13), (blocks, 1), jnp.float32, -0.7, 0.7))
    row_scale = jnp.exp(jax.random.uniform(jax.random.fold_in(key, 14), (ROWS, 1), jnp.float32, -0.5, 0.5))
    scaled = jnp.repeat(block_scale, R_DEV, axis=0) * row_scale
    mixed = jnp.dot(base_rows * scaled, column_mix(key), precision=lax.Precision.HIGHEST, preferred_element_type=jnp.float32)
    return mixed / jnp.sqrt(jnp.float32(ROWS))


def draw_matrix(key, part):
    return shared_rows(key)


def draw_grad_out(key, part):
    noise_rows = jax.random.normal(jax.random.fold_in(key, 21), (ROWS, N), jnp.float32)
    return 0.01 * (noise_rows + 0.03 * jnp.sqrt(jnp.float32(ROWS)) * shared_rows(key))


def normal_values(stream_key, dims, scale, most, held_as=jnp.bfloat16):
    entries = jax.random.normal(stream_key, dims, jnp.float32) * scale
    return jnp.minimum(jnp.maximum(entries, -most), most).astype(held_as)


def setup_inputs(seed: int = 0) -> dict:
    arg_keys = jax.random.split(jax.random.key(seed), 4)
    return {
        "matrix": draw_matrix(jax.random.fold_in(arg_keys[3], 71), 0),
        "grad_out": draw_grad_out(jax.random.fold_in(arg_keys[3], 71), 0),
        "grad_factor": normal_values(arg_keys[2], (N, N), 1.0, 6.0, jnp.float32),
    }


shift_frac = 0.02

def full_dot(left, right):
    return jnp.dot(left.astype(jnp.float32), right.astype(jnp.float32), precision=lax.Precision.HIGHEST, preferred_element_type=jnp.float32)

def inner_gram(left, right):
    return lax.dot_general(left.astype(jnp.float32), right.astype(jnp.float32), (((0,), (0,)), ((), ())), precision=lax.Precision.HIGHEST, preferred_element_type=jnp.float32)

def cholesky_adjoint(lower_fac, lower_inv, lower_grad):
    product = full_dot(lower_fac.T, lower_grad)
    phi_part = jnp.tril(product) - 0.5 * jnp.diag(jnp.diag(product))
    sandwich = full_dot(full_dot(lower_inv.T, phi_part), lower_inv)
    return 0.5 * (sandwich + sandwich.T)

def factor_grads(uppers, grad_factor):
    count = len(uppers)
    result = []
    for section_index in range(count):
        middle = grad_factor
        for later in range(section_index + 1, count):
            middle = full_dot(uppers[later].T, middle)
        for earlier in range(section_index - 1, -1, -1):
            middle = full_dot(middle, uppers[earlier].T)
        result.append(middle)
    return result

def reference(matrix, grad_out, grad_factor):
    width = matrix.shape[1]
    rate = shift_frac / width
    identity = jnp.eye(width, dtype=jnp.float32)
    current = matrix
    saved = []
    for section_index in range(SECTIONS):
        summed = inner_gram(current, current)
        shift_val = rate * jnp.trace(summed)
        lower_fac = jnp.linalg.cholesky(summed + shift_val * identity)
        lower_inv = lax.linalg.triangular_solve(lower_fac, identity, left_side=True, lower=True)
        following = full_dot(current, lower_inv.T)
        saved.append((current, following, lower_fac, lower_inv))
        current = following
    uppers = [item[2].T for item in saved]
    fac_grads = factor_grads(uppers, grad_factor)
    q_grad = grad_out
    for section_index in range(SECTIONS - 1, -1, -1):
        before, after, lower_fac, lower_inv = saved[section_index]
        crossed = inner_gram(after, q_grad)
        total_grad = fac_grads[section_index] - full_dot(crossed, lower_inv)
        gram_grad = cholesky_adjoint(lower_fac, lower_inv, jnp.tril(total_grad.T))
        gram_grad = gram_grad + rate * jnp.trace(gram_grad) * identity
        q_grad = full_dot(q_grad, lower_inv) + 2.0 * full_dot(before, gram_grad)
    return q_grad
```

```python
import jax
import jax.numpy as jnp
from jax import lax
from jax.experimental import pallas as pl
from jax.experimental.pallas import tpu as pltpu
from jax.sharding import PartitionSpec as P

SECTIONS = 2
BLOCK = 128
PANEL = 8
CHUNKS = 8

shift_frac = 0.02


f32 = jnp.float32


def dot(left, right, left_dim=1, right_dim=0):
    return lax.dot_general(
        left,
        right,
        (((left_dim,), (right_dim,)), ((), ())),
        precision=lax.Precision.HIGHEST,
        preferred_element_type=f32,
    )


def dot_nt(left, right):
    return dot(left, right, 1, 1)


def dot_tn(left, right):
    return dot(left, right, 0, 0)


def row_col(shape):
    return lax.broadcasted_iota(jnp.int32, shape, 0), lax.broadcasted_iota(jnp.int32, shape, 1)


def mirror_lower(block):
    row, col = row_col(block.shape)
    return jnp.where(row >= col, block, block.T)


def mirror_upper(block):
    row, col = row_col(block.shape)
    return jnp.where(row <= col, block, block.T)


def factor_block(sym, upper_ref, inv_ref):
    size = sym.shape[0]
    count = size // PANEL
    row, col = row_col((PANEL, size))
    rest = [sym[PANEL * i : PANEL * (i + 1), :] for i in range(count)]
    unit = [jnp.where(col == row + PANEL * i, 1.0, 0.0).astype(f32) for i in range(count)]

    def over_lanes(value, lane):
        return jnp.broadcast_to(value[:, lane : lane + 1], (PANEL, size))

    def over_sublanes(value, sublane):
        return jnp.broadcast_to(value[sublane : sublane + 1, :], (PANEL, size))

    for k in range(count):
        base = PANEL * k
        spread = [over_lanes(rest[k], base + c) for c in range(PANEL)]
        top, top_unit = rest[k], unit[k]
        uppers, invs, scales, pairs = [], [], [], {}
        upper_out = inv_out = None
        for j in range(PANEL):
            scale = lax.rsqrt(over_sublanes(spread[j], j))
            scales.append(scale)
            lower = spread[j] * scale
            upper_row = over_sublanes(top, j) * scale
            inv_row = over_sublanes(top_unit, j) * scale
            uppers.append(upper_row)
            invs.append(inv_row)
            for c in range(j + 1, PANEL):
                pairs[j, c] = over_sublanes(spread[c], j) * scale
                spread[c] = spread[c] - lower * pairs[j, c]
            upper_out = upper_row if j == 0 else jnp.where(row == j, upper_row, upper_out)
            inv_out = inv_row if j == 0 else jnp.where(row == j, inv_row, inv_out)
            if j < PANEL - 1:
                top = top - lower * upper_row
                top_unit = top_unit - lower * inv_row
        upper_ref[base : base + PANEL, :] = jnp.where(col >= row + base, upper_out, 0.0)
        inv_ref[base : base + PANEL, :] = inv_out
        for i in range(k + 1, count):
            below = [over_lanes(rest[i], base + c) for c in range(PANEL)]
            value, value_unit = rest[i], unit[i]
            for j in range(PANEL):
                lower = below[j] * scales[j]
                for c in range(j + 1, PANEL):
                    below[c] = below[c] - lower * pairs[j, c]
                value = value - lower * uppers[j]
                value_unit = value_unit - lower * invs[j]
            rest[i], unit[i] = value, value_unit


def cholesky_inverse(sym_ref, lower_ref, inv_ref, tile_ref):
    width = sym_ref.shape[0]
    count = width // BLOCK
    for b in range(count):
        lo, hi = b * BLOCK, (b + 1) * BLOCK
        diag = inv_ref.at[lo:hi, lo:hi]
        factor_block(sym_ref[lo:hi, lo:hi], tile_ref, diag)
        lower_ref[lo:hi, lo:hi] = tile_ref[...].T
        if hi < width:
            zero = jnp.zeros((BLOCK, width - hi), f32)
            lower_ref[lo:hi, hi:] = zero
            inv_ref[lo:hi, hi:] = zero
            below = dot_nt(sym_ref[hi:, lo:hi], diag[...])
            lower_ref[hi:, lo:hi] = below
            for j in range(b + 1, count):
                jlo, jhi = j * BLOCK, (j + 1) * BLOCK
                sym_ref[jlo:, jlo:jhi] -= dot_nt(below[jlo - hi :], below[jlo - hi : jhi - hi])
        if b:
            inner = dot(lower_ref[lo:hi, :lo], inv_ref[:lo, :lo])
            inv_ref[lo:hi, :lo] = -dot(diag[...], inner)


def shift_diagonal(sym_ref, rate):
    width = sym_ref.shape[0]
    row, col = row_col((BLOCK, BLOCK))
    on_diag = row == col
    total = jnp.zeros((1, 1), f32)
    for b in range(width // BLOCK):
        lo, hi = b * BLOCK, (b + 1) * BLOCK
        total += jnp.sum(jnp.where(on_diag, sym_ref[lo:hi, lo:hi], 0.0), keepdims=True)
    shift = total * rate
    for b in range(width // BLOCK):
        lo, hi = b * BLOCK, (b + 1) * BLOCK
        sym_ref[lo:hi, lo:hi] += jnp.where(on_diag, jnp.broadcast_to(shift, (BLOCK, BLOCK)), 0.0)


def packed_rows(width):
    part = width // CHUNKS
    return part, part + PANEL


def gram_kernel(matrix_ref, grad_ref, out_ref):
    matrix, grad = matrix_ref[...], grad_ref[...]
    width = matrix.shape[1]
    turned = matrix.T
    part, piece = packed_rows(width)
    diag = jnp.sum(matrix * grad, axis=0, keepdims=True)
    gram = dot(turned, matrix)
    cross = dot(turned, grad)
    row, col = row_col((width, width))
    packed = jnp.where(row >= col, gram, cross)
    for c in range(CHUNKS):
        out_ref[c * piece : c * piece + part, :] = packed[c * part : (c + 1) * part, :]
        out_ref[c * piece + part : (c + 1) * piece, :] = jnp.broadcast_to(diag, (PANEL, width))


def first_kernel(packed_ref, matrix_ref, lower_ref, inv_ref, cross_ref, gram_ref, sym_ref, tile_ref, *, rate):
    width = matrix_ref.shape[1]
    part, piece = packed_rows(width)
    for c in range(CHUNKS):
        sym_ref[c * part : (c + 1) * part, :] = packed_ref[c * piece : c * piece + part, :]
    row, col = row_col((width, width))
    diag = jnp.broadcast_to(packed_ref[part : part + 1, :], (width, width))
    cross_ref[...] = jnp.where(row < col, sym_ref[...], jnp.where(row == col, diag, 0.0))
    for b in range(width // BLOCK):
        lo, hi = b * BLOCK, (b + 1) * BLOCK
        sym_ref[lo:hi, lo:hi] = mirror_lower(sym_ref[lo:hi, lo:hi])
    shift_diagonal(sym_ref, rate)
    cholesky_inverse(sym_ref, lower_ref, inv_ref, tile_ref)
    following = dot_nt(inv_ref[...], matrix_ref[...])
    place = 0
    for j in range(width // BLOCK):
        lo, hi = j * BLOCK, (j + 1) * BLOCK
        column = dot_nt(following[lo:], following[lo:hi])
        for i in range(j, width // BLOCK):
            gram_ref[place] = column[i * BLOCK - lo : (i + 1) * BLOCK - lo]
            place += 1


def middle_kernel(lower_ref, inv_ref, cross_ref, factor_ref, inv_cross_ref, factor_lower_ref):
    inv_cross_ref[...] = dot(inv_ref[...], cross_ref[...])
    factor_lower_ref[...] = dot(factor_ref[...], lower_ref[...])


def upper_part(value):
    row, col = row_col(value.shape)
    return jnp.where(row <= col, value, 0.0)


def last_kernel(
    gram_ref, lower1_ref, inv1_ref, inv_cross_ref, factor_lower_ref, factor_ref, matrix_ref, grad_ref, out_ref,
    sym_ref, lower2_ref, inv2_ref, full_ref, tile_ref, *, rate
):
    width = matrix_ref.shape[1]
    count = width // BLOCK
    row, col = row_col((width, width))
    place = 0
    for j in range(count):
        lo, hi = j * BLOCK, (j + 1) * BLOCK
        for i in range(j, count):
            block = gram_ref[place]
            place += 1
            sym_ref[i * BLOCK : (i + 1) * BLOCK, lo:hi] = block
            full_ref[i * BLOCK : (i + 1) * BLOCK, lo:hi] = block
            if i > j:
                full_ref[lo:hi, i * BLOCK : (i + 1) * BLOCK] = block.T
    shift_diagonal(sym_ref, rate)
    cholesky_inverse(sym_ref, lower2_ref, inv2_ref, tile_ref)
    inv1, inv2, lower2 = inv1_ref[...], inv2_ref[...], lower2_ref[...]
    both = dot(inv2, inv1)
    half = dot(inv_cross_ref[...], inv2)
    second = upper_part(factor_lower_ref[...] - dot(inv2, half))
    middle = 0.5 * mirror_upper(dot(second, lower2))
    side = dot(middle, inv2)
    weight = dot_tn(inv2, side) + jnp.where(row == col, rate * jnp.sum(side * inv2, keepdims=True), 0.0)
    crossed = half + 2.0 * dot(full_ref[...], weight)
    first = upper_part(dot(lower2, factor_ref[...]) - dot(crossed, inv1))
    middle = 0.5 * mirror_upper(dot(first, lower1_ref[...]))
    side = dot(middle, inv1)
    trace = rate * jnp.sum(side * inv1, keepdims=True)
    onto = dot_tn(inv1, side + dot(weight, inv1)) + jnp.where(row == col, trace, 0.0)
    out_ref[...] = dot(grad_ref[...], both) + 2.0 * dot(matrix_ref[...], onto)


def exchange_levels(count):
    levels, stride = [], 1
    while stride < count:
        left = count // stride
        size = left if left <= 8 and levels else min(4, left)
        levels.append((stride, size))
        stride *= size
    return levels


def sum_over_devices(value, counts):
    rows_count, sub_count = counts
    levels = [("sub", 1, sub_count)] + [("rows", s, n) for s, n in exchange_levels(rows_count)]
    totals = {"rows": rows_count, "sub": sub_count}

    def send(array, axis, change):
        return lax.ppermute(array, axis, [(i, i ^ change) for i in range(totals[axis])])

    def tree(values):
        while len(values) > 1:
            values = [values[i] + values[i + 1] for i in range(0, len(values), 2)]
        return values[0]

    shape = value.shape[1:]
    for axis, stride, size in levels[:-1]:
        spot = (lax.axis_index(axis) // stride) % size
        pieces = value.reshape((size, value.shape[0] // size) + shape)
        got = [lax.dynamic_index_in_dim(pieces, spot, 0, False)]
        for other in range(1, size):
            got.append(send(lax.dynamic_index_in_dim(pieces, spot ^ other, 0, False), axis, other * stride))
        value = tree(got)
    axis, stride, size = levels[-1]
    value = tree([value] + [send(value, axis, other * stride) for other in range(1, size)])
    for axis, stride, size in levels[-2::-1]:
        spot = (lax.axis_index(axis) // stride) % size
        got = [value] + [send(value, axis, other * stride) for other in range(1, size)]
        pieces = jnp.zeros((size,) + value.shape, f32)
        for other in range(size):
            pieces = lax.dynamic_update_index_in_dim(pieces, got[other], spot ^ other, 0)
        value = pieces.reshape((size * value.shape[0],) + shape)
    return value


def call(kernel, out_shapes, scratch_shapes, *operands):
    vmem = pl.BlockSpec(memory_space=pltpu.VMEM)
    shapes = [jax.ShapeDtypeStruct(s, f32) for s in out_shapes]
    return pl.pallas_call(
        kernel,
        out_shape=shapes,
        in_specs=[vmem] * len(operands),
        out_specs=[vmem] * len(shapes),
        scratch_shapes=[pltpu.VMEM(s, f32) for s in scratch_shapes],
    )(*operands)


def solution(mesh):
    counts = (mesh.shape["rows"], mesh.shape["sub"])

    def per_device(matrix, grad_out, grad_factor):
        width = matrix.shape[1]
        rate = shift_frac / width
        blocks = width // BLOCK
        lower_blocks = blocks * (blocks + 1) // 2
        square, tile = (width, width), (BLOCK, BLOCK)

        def first(*refs):
            first_kernel(*refs, rate=rate)

        def last(*refs):
            last_kernel(*refs, rate=rate)

        (packed,) = call(gram_kernel, [(CHUNKS * packed_rows(width)[1], width)], [], matrix, grad_out)
        packed = sum_over_devices(packed, counts)
        lower1, inv1, cross, gram = call(
            first, [square, square, square, (lower_blocks, BLOCK, BLOCK)], [square, tile], packed, matrix
        )
        gram = sum_over_devices(gram.reshape(lower_blocks * BLOCK, BLOCK), counts).reshape(gram.shape)
        inv_cross, factor_lower = call(middle_kernel, [square, square], [], lower1, inv1, cross, grad_factor)
        (out,) = call(
            last,
            [matrix.shape],
            [square, square, square, square, tile],
            gram, lower1, inv1, inv_cross, factor_lower, grad_factor, matrix, grad_out,
        )
        return out

    placed = (P(("rows", "sub"), None), P(("rows", "sub"), None), P())
    return jax.shard_map(
        per_device, mesh=mesh, in_specs=placed, out_specs=P(("rows", "sub"), None), check_vma=False
    )
```

```python
import jax
import jax.numpy as jnp
from jax import lax
from jax.experimental import pallas as pl
from jax.experimental.pallas import tpu as pltpu
from jax.sharding import PartitionSpec as P

SECTIONS = 2
BLOCK = 128
PANEL = 8
CHUNKS = 8
SLICES = 4

shift_frac = 0.02


f32 = jnp.float32


def thirds(value):
    high = value.astype(jnp.bfloat16)
    value = value - high.astype(f32)
    middle = value.astype(jnp.bfloat16)
    return high, middle, (value - middle.astype(f32)).astype(jnp.bfloat16)


def dot(left, right, left_dim=1, right_dim=0):
    lh, lm, ll = thirds(left)
    rh, rm, rl = thirds(right)

    def side_by_side(lefts, rights):
        return lax.dot_general(
            jnp.concatenate(lefts, axis=left_dim),
            jnp.concatenate(rights, axis=right_dim),
            (((left_dim,), (right_dim,)), ((), ())),
            preferred_element_type=f32,
        )

    return side_by_side([lh, lm, lh, ll], [rl, rm, rm, rh]) + side_by_side([lm, lh], [rh, rh])


def dot_nt(left, right):
    return dot(left, right, 1, 1)


def row_col(shape):
    return lax.broadcasted_iota(jnp.int32, shape, 0), lax.broadcasted_iota(jnp.int32, shape, 1)


def mirror_lower(block):
    row, col = row_col(block.shape)
    return jnp.where(row >= col, block, block.T)


def mirror_upper(block):
    row, col = row_col(block.shape)
    return jnp.where(row <= col, block, block.T)


def factor_block(sym_ref, upper_ref, inv_ref):
    size = sym_ref.shape[0]
    count = size // PANEL
    row, col = row_col((PANEL, size))
    rest = [sym_ref[PANEL * i : PANEL * (i + 1), :] for i in range(count)]
    unit = [jnp.where(col == row + PANEL * i, 1.0, 0.0).astype(f32) for i in range(count)]

    def over_lanes(value, lane):
        return jnp.broadcast_to(value[:, lane : lane + 1], (PANEL, size))

    def over_sublanes(value, sublane):
        return jnp.broadcast_to(value[sublane : sublane + 1, :], (PANEL, size))

    def columns_of(value, base):
        return [over_lanes(value, base + c) for c in range(PANEL)]

    spread = columns_of(rest[0], 0)
    for k in range(count):
        base = PANEL * k
        more = k + 1 < count
        if more:
            ahead = columns_of(rest[k + 1], base + PANEL)
            near = columns_of(rest[k + 1], base)
        uppers, invs, scales, pairs = [], [], [], {}
        upper_out = inv_out = None
        for j in range(PANEL):
            scale = lax.rsqrt(over_sublanes(spread[j], j))
            scales.append(scale)
            lower = spread[j] * scale
            upper_row = over_sublanes(rest[k], j) * scale
            inv_row = over_sublanes(unit[k], j) * scale
            upper_out = upper_row if j == 0 else jnp.where(row == j, upper_row, upper_out)
            inv_out = inv_row if j == 0 else jnp.where(row == j, inv_row, inv_out)
            for c in range(j + 1, PANEL):
                pairs[j, c] = over_sublanes(spread[c], j) * scale
                spread[c] = spread[c] - lower * pairs[j, c]
            if j < PANEL - 1:
                rest[k] = rest[k] - lower * upper_row
                unit[k] = unit[k] - lower * inv_row
            if more:
                lower = near[j] * scale
                for c in range(j + 1, PANEL):
                    near[c] = near[c] - lower * pairs[j, c]
                for c in range(PANEL):
                    ahead[c] = ahead[c] - lower * over_sublanes(lower, c)
                rest[k + 1] = rest[k + 1] - lower * upper_row
                unit[k + 1] = unit[k + 1] - lower * inv_row
            uppers.append(upper_row)
            invs.append(inv_row)
        upper_ref[base : base + PANEL, :] = jnp.where(col >= row + base, upper_out, 0.0)
        inv_ref[base : base + PANEL, :] = inv_out
        if more:
            spread = ahead
        for i in range(k + 2, count):
            below = columns_of(rest[i], base)
            for j in range(PANEL):
                lower = below[j] * scales[j]
                for c in range(j + 1, PANEL):
                    below[c] = below[c] - lower * pairs[j, c]
                rest[i] = rest[i] - lower * uppers[j]
                unit[i] = unit[i] - lower * invs[j]


def cholesky_inverse(sym_ref, lower_ref, inv_ref, work_ref, tile_ref, unit_ref):
    width = sym_ref.shape[0]
    count = width // BLOCK
    work_ref[...] = sym_ref[:BLOCK, :BLOCK]

    def step(b, carry):
        factor_block(work_ref, tile_ref, unit_ref)
        for place in range(count):
            pl.when(b == place)(lambda place=place: after_block(place))
        return carry

    def after_block(b):
        lo, hi = b * BLOCK, (b + 1) * BLOCK
        unit = unit_ref[...]
        inv_ref[lo:hi, lo:hi] = unit
        lower_ref[lo:hi, lo:hi] = tile_ref[...].T
        if hi < width:
            zero = jnp.zeros((BLOCK, width - hi), f32)
            lower_ref[lo:hi, hi:] = zero
            inv_ref[lo:hi, hi:] = zero
            below = dot_nt(sym_ref[hi:, lo:hi], unit)
            lower_ref[hi:, lo:hi] = below
            left = sym_ref[hi : hi + BLOCK, hi : hi + BLOCK] - dot_nt(below[:BLOCK], below[:BLOCK])
            work_ref[...] = mirror_lower(left)
            for j in range(b + 1, count):
                jlo, jhi = j * BLOCK, (j + 1) * BLOCK
                start = jhi if j == b + 1 else jlo
                if start < width:
                    sym_ref[start:, jlo:jhi] -= dot_nt(below[start - hi :], below[jlo - hi : jhi - hi])
        if b:
            inner = dot(lower_ref[lo:hi, :lo], inv_ref[:lo, :lo])
            inv_ref[lo:hi, :lo] = -dot(unit, inner)

    lax.fori_loop(0, count, step, 0)


def two_sum(left, right):
    total = left + right
    part = total - left
    return total, (left - (total - part)) + (right - part)


def exact_terms(value, triangular):
    anchor = jnp.max(jnp.abs(value), axis=1, keepdims=True) * (1.5 * 2.0**16)
    parts = []
    for k in range(SLICES):
        grid = jnp.broadcast_to(anchor * 2.0 ** (-8 * k), value.shape)
        part = (value + grid) - grid
        value = value - part
        parts.append(part.astype(jnp.bfloat16))
    for lo in range(0, value.shape[0], BLOCK):
        hi = lo + BLOCK
        inner = hi if triangular else value.shape[1]
        left = jnp.concatenate([part[lo:, :inner] for part in parts], axis=1)
        right = jnp.concatenate([part[lo:hi, :inner] for part in parts[::-1]], axis=1)
        terms = []
        for k in range(SLICES + 1):
            start, stop = max(0, k + 1 - SLICES) * inner, min(k + 1, SLICES) * inner
            back = max(0, SLICES - 1 - k) * inner
            terms.append(
                lax.dot_general(
                    left[:, start:stop],
                    right[:, back : back + stop - start],
                    (((1,), (1,)), ((), ())),
                    preferred_element_type=f32,
                )
            )
        yield terms


def halves(value):
    high = value.astype(jnp.bfloat16)
    return high, (value - high.astype(f32)).astype(jnp.bfloat16)


def dot3(left, right, left_dim=1, right_dim=0):
    lh, ll = halves(left)
    rh, rl = halves(right)
    return lax.dot_general(
        jnp.concatenate([lh, lh, ll], axis=left_dim),
        jnp.concatenate([rh, rl, rh], axis=right_dim),
        (((left_dim,), (right_dim,)), ((), ())),
        preferred_element_type=f32,
    )


def lower_blocks(width):
    count = width // BLOCK
    return [(i, j) for j in range(count) for i in range(j, count)]


def upper_blocks(width):
    return [(j, i) for i, j in lower_blocks(width) if i > j]


def pieces_of(width):
    low = len(lower_blocks(width))
    return low, low + len(upper_blocks(width)), 2 * low + len(upper_blocks(width))


def span(block):
    return slice(block * BLOCK, (block + 1) * BLOCK)


def gram_kernel(matrix_ref, grad_ref, out_ref):
    matrix, grad = matrix_ref[...], grad_ref[...]
    width = matrix.shape[1]
    count = width // BLOCK
    turned = matrix.T
    rows = BLOCK // CHUNKS
    row, col = row_col((BLOCK, BLOCK))
    lower, upper = lower_blocks(width), upper_blocks(width)
    low_at, upper_at = pieces_of(width)[1], pieces_of(width)[0]

    def put(piece, block):
        for c in range(CHUNKS):
            out_ref[c, piece] = block[c * rows : (c + 1) * rows, :]

    diag = jnp.sum(matrix * grad, axis=0, keepdims=True)
    tail = jnp.concatenate([diag[:, span(b)] for b in range(count)] + [jnp.zeros((rows - count, BLOCK), f32)], axis=0)
    for c in range(CHUNKS):
        out_ref[c, pieces_of(width)[2]] = tail
    crosses = [dot(turned[: (j + 1) * BLOCK], grad[:, span(j)]) for j in range(count)]
    for j, terms in enumerate(exact_terms(turned, False)):
        high, error = two_sum(terms[0], terms[1])
        low = error
        for term in terms[2:]:
            low = low + term
        total = high + low
        low = low - (total - high)
        for i in range(j, count):
            place = lower.index((i, j))
            here = slice((i - j) * BLOCK, (i - j + 1) * BLOCK)
            block = total[here]
            if i == j:
                block = jnp.where(row >= col, block, crosses[j][span(j)])
            put(place, block)
            put(low_at + place, low[here])
        for i in range(j):
            put(upper_at + upper.index((i, j)), crosses[j][span(i)])


def upper_part(value):
    row, col = row_col(value.shape)
    return jnp.where(row <= col, value, 0.0)


def main_kernel(
    packed_ref, factor_hbm, matrix_hbm, grad_hbm, out_ref,
    sym_ref, cross_ref, lower1_ref, inv1_ref, lower2_ref, inv2_ref, full_ref, spread_ref, early_ref, factor_ref,
    work_ref, tile_ref, unit_ref, matrix_ref, grad_ref, before_ref, arrived, *, rate
):
    arrivals = [
        pltpu.make_async_copy(source, target, arrived.at[k])
        for k, (source, target) in enumerate(
            [(factor_hbm, factor_ref), (matrix_hbm, matrix_ref), (grad_hbm, grad_ref)]
        )
    ]
    for arrival in arrivals:
        arrival.start()
    width = matrix_ref.shape[1]
    count = width // BLOCK
    rows = BLOCK // CHUNKS
    row, col = row_col((BLOCK, BLOCK))
    on_diag = row == col
    lower, upper = lower_blocks(width), upper_blocks(width)
    upper_at, low_at, diag_at = pieces_of(width)

    def block_of(piece):
        return jnp.concatenate([packed_ref[c, piece] for c in range(CHUNKS)], axis=0)

    def trace_of(ref):
        total = jnp.zeros((1, 1), f32)
        for b in range(count):
            total += jnp.sum(jnp.where(on_diag, ref[span(b), span(b)], 0.0), keepdims=True)
        return total

    def shifted(block, shift):
        return block + jnp.where(on_diag, jnp.broadcast_to(shift, block.shape), 0.0)

    for place, (i, j) in enumerate(lower):
        block = block_of(place)
        if i == j:
            diag = jnp.broadcast_to(packed_ref[0, diag_at, i : i + 1, :], block.shape)
            cross_ref[span(i), span(i)] = jnp.where(row < col, block, jnp.where(on_diag, diag, 0.0))
            block = mirror_lower(block)
        else:
            cross_ref[span(i), span(j)] = jnp.zeros_like(block)
        sym_ref[span(i), span(j)] = block
    for place, (i, j) in enumerate(upper):
        cross_ref[span(i), span(j)] = block_of(upper_at + place)
    shift1 = trace_of(sym_ref) * rate
    for b in range(count):
        sym_ref[span(b), span(b)] = shifted(sym_ref[span(b), span(b)], shift1)
    cholesky_inverse(sym_ref, lower1_ref, inv1_ref, work_ref, tile_ref, unit_ref)

    for j, terms in enumerate(exact_terms(lower1_ref[...], True)):
        for i in range(j, count):
            place = lower.index((i, j))
            here = slice((i - j) * BLOCK, (i - j + 1) * BLOCK)
            high = block_of(place)
            rest = block_of(low_at + place)
            if i == j:
                high, error = two_sum(high, jnp.where(on_diag, jnp.broadcast_to(shift1, high.shape), 0.0))
                rest = rest + error
            high, error = two_sum(high, -terms[0][here])
            high, error2 = two_sum(high, -terms[1][here])
            rest = rest + (error + error2)
            for term in terms[2:]:
                rest = rest - term[here]
            block = high + rest
            if i == j:
                block = mirror_lower(block)
            else:
                full_ref[span(j), span(i)] = block.T
            full_ref[span(i), span(j)] = block
    inv1 = inv1_ref[...]
    spread = dot3(inv1, full_ref[...])
    for arrival in arrivals:
        arrival.wait()
    early_ref[...] = dot3(factor_ref[...], lower1_ref[...])
    before_ref[...] = dot_nt(matrix_ref[...], inv1)
    cross_ref[...] = dot(inv1, cross_ref[...])
    for j in range(count):
        lo = j * BLOCK
        spread_ref[lo:, span(j)] = dot_nt(inv1[lo:], inv1[span(j)])
        column = dot3(spread[lo:], inv1[span(j)], 1, 1) - jnp.broadcast_to(shift1, (width - lo, BLOCK)) * spread_ref[lo:, span(j)]
        for i in range(j, count):
            block = column[(i - j) * BLOCK : (i - j + 1) * BLOCK]
            if i == j:
                block = mirror_lower(jnp.where(on_diag, block + 1.0, block))
            else:
                full_ref[span(j), span(i)] = block.T
            full_ref[span(i), span(j)] = block
    shift2 = trace_of(full_ref) * rate
    for i, j in lower:
        block = full_ref[span(i), span(j)]
        sym_ref[span(i), span(j)] = shifted(block, shift2) if i == j else block
    cholesky_inverse(sym_ref, lower2_ref, inv2_ref, work_ref, tile_ref, unit_ref)

    inv1, inv2, lower1, lower2 = inv1_ref[...], inv2_ref[...], lower1_ref[...], lower2_ref[...]
    wide_row, wide_col = row_col((width, width))
    half = dot3(cross_ref[...], inv2)
    second = upper_part(early_ref[...] - dot3(inv2, half))
    middle = 0.5 * mirror_upper(dot3(second, lower2))
    side = dot3(middle, inv2)
    weight = dot3(inv2, side, 0, 0) + jnp.where(wide_row == wide_col, rate * jnp.sum(side * inv2, keepdims=True), 0.0)
    crossed = half + 2.0 * dot3(full_ref[...], weight)
    first = upper_part(dot3(lower2, factor_ref[...]) - dot3(crossed, inv1))
    middle = 0.5 * mirror_upper(dot3(first, lower1))
    trace = jnp.zeros((1, 1), f32)
    for i, j in lower:
        part = jnp.sum(middle[span(i), span(j)] * spread_ref[span(i), span(j)], keepdims=True)
        trace += part if i == j else 2.0 * part
    through = dot3(grad_ref[...], inv2) + 2.0 * dot3(before_ref[...], weight + middle)
    out_ref[...] = dot3(through, inv1) + (2.0 * rate) * trace * matrix_ref[...]


def exchange_levels(count):
    levels, stride = [], 1
    while stride < count:
        left = count // stride
        size = left if left <= 8 and levels else min(4, left)
        levels.append((stride, size))
        stride *= size
    return levels


def sum_over_devices(value, counts, low):
    rows_count, sub_count = counts
    levels = [("sub", 1, sub_count)] + [("rows", s, n) for s, n in exchange_levels(rows_count)]
    totals = {"rows": rows_count, "sub": sub_count}
    many, start = low

    def send(array, axis, change):
        return lax.ppermute(array, axis, [(i, i ^ change) for i in range(totals[axis])])

    def swap(mine, axis, stride):
        mine = lax.optimization_barrier(tuple(mine))
        return lax.optimization_barrier(
            (mine[0],) + tuple(send(mine[k], axis, k * stride) for k in range(1, len(mine)))
        )

    def add(left, right):
        total, error = two_sum(left, right)
        after = total.shape[-3] - start - many
        pad = [(0, 0)] * (total.ndim - 3) + [(start, after), (0, 0), (0, 0)]
        return total + jnp.pad(error[..., :many, :, :], pad)

    def tree(values):
        while len(values) > 1:
            values = [add(values[i], values[i + 1]) for i in range(0, len(values), 2)]
        return values[0]

    split = []
    for axis, stride, size in levels:
        if value.shape[0] % size == 0:
            spot = (lax.axis_index(axis) // stride) % size
            pieces = value.reshape((size, value.shape[0] // size) + value.shape[1:])
            mine = [lax.dynamic_index_in_dim(pieces, spot ^ other, 0, False) for other in range(size)]
            split.append((axis, stride, size, spot))
            value = tree(swap(mine, axis, stride))
        else:
            change = 1
            while change < size:
                value = add(value, send(value, axis, change * stride))
                change = 2 * change + 1
    for axis, stride, size, spot in split[::-1]:
        got = swap([value] * size, axis, stride)
        pieces = jnp.zeros((size,) + value.shape, f32)
        for other in range(size):
            pieces = lax.dynamic_update_index_in_dim(pieces, got[other], spot ^ other, 0)
        value = pieces.reshape((size * value.shape[0],) + value.shape[1:])
    return value


def call(kernel, out_shapes, scratch_shapes, *operands, spaces=None):
    vmem = pl.BlockSpec(memory_space=pltpu.VMEM)
    return pl.pallas_call(
        kernel,
        out_shape=out_shapes,
        in_specs=spaces or [vmem] * len(operands),
        out_specs=[vmem] * len(out_shapes),
        scratch_shapes=scratch_shapes,
    )(*operands)


def run_gram(matrix, grad_out):
    shape = (CHUNKS, pieces_of(matrix.shape[1])[2] + 1, BLOCK // CHUNKS, BLOCK)
    return call(gram_kernel, [pltpu.VMEM(shape, f32)], [], matrix, grad_out)[0]


def run_main(packed, grad_factor, matrix, grad_out):
    width = matrix.shape[1]
    square, tile, rows = [pltpu.VMEM(s, f32) for s in ((width, width), (BLOCK, BLOCK), matrix.shape)]

    def main(*refs):
        main_kernel(*refs, rate=shift_frac / width)

    packed = pltpu.with_memory_space_constraint(packed, pltpu.VMEM)
    scratch = [square] * 10 + [tile] * 3 + [rows] * 3 + [pltpu.SemaphoreType.DMA((3,))]
    spaces = [pl.BlockSpec(memory_space=pltpu.VMEM)] + [pl.BlockSpec(memory_space=pl.ANY)] * 3
    out = jax.ShapeDtypeStruct(matrix.shape, f32)
    return call(main, [out], scratch, packed, grad_factor, matrix, grad_out, spaces=spaces)[0]


def solution(mesh):
    counts = (mesh.shape["rows"], mesh.shape["sub"])

    def per_device(matrix, grad_out, grad_factor):
        many, start, _ = pieces_of(matrix.shape[1])
        packed = sum_over_devices(run_gram(matrix, grad_out), counts, (many, start))
        return run_main(packed, grad_factor, matrix, grad_out)

    placed = (P(("rows", "sub"), None), P(("rows", "sub"), None), P())
    return jax.shard_map(
        per_device, mesh=mesh, in_specs=placed, out_specs=P(("rows", "sub"), None), check_vma=False
    )
```

```python
import jax
import jax.numpy as jnp
from jax import lax
from jax.experimental import pallas as pl
from jax.experimental.pallas import tpu as pltpu
from jax.sharding import PartitionSpec as P

SECTIONS = 2
BLOCK = 128
PANEL = 8
CHUNKS = 8
SLICES = 4

shift_frac = 0.02


f32 = jnp.float32


def thirds(value):
    high = value.astype(jnp.bfloat16)
    value = value - high.astype(f32)
    middle = value.astype(jnp.bfloat16)
    return high, middle, (value - middle.astype(f32)).astype(jnp.bfloat16)


def dot(left, right, left_dim=1, right_dim=0):
    lh, lm, ll = thirds(left)
    rh, rm, rl = thirds(right)

    def side_by_side(lefts, rights):
        return lax.dot_general(
            jnp.concatenate(lefts, axis=left_dim),
            jnp.concatenate(rights, axis=right_dim),
            (((left_dim,), (right_dim,)), ((), ())),
            preferred_element_type=f32,
        )

    return side_by_side([lh, lm, lh, ll], [rl, rm, rm, rh]) + side_by_side([lm, lh], [rh, rh])


def dot_nt(left, right):
    return dot(left, right, 1, 1)


def row_col(shape):
    return lax.broadcasted_iota(jnp.int32, shape, 0), lax.broadcasted_iota(jnp.int32, shape, 1)


def mirror_lower(block):
    row, col = row_col(block.shape)
    return jnp.where(row >= col, block, block.T)


def mirror_upper(block):
    row, col = row_col(block.shape)
    return jnp.where(row <= col, block, block.T)


def factor_block(sym_ref, upper_ref, corner_ref, inv_ref):
    size = sym_ref.shape[0]
    count = size // PANEL
    row, col = row_col((PANEL, size))
    rows = [sym_ref[PANEL * i : PANEL * (i + 1), :] for i in range(count)]

    def over_lanes(value, lane):
        return jnp.broadcast_to(value[:, lane : lane + 1], (PANEL, size))

    def over_sublanes(value, sublane):
        return jnp.broadcast_to(value[sublane : sublane + 1, :], (PANEL, size))

    def columns_of(value, base):
        return [over_lanes(value, base + c) for c in range(PANEL)]

    spread = columns_of(rows[0], 0)
    for k in range(count):
        base = PANEL * k
        more = k + 1 < count
        in_panel = (col >= base) & (col < base + PANEL)
        if more:
            ahead = columns_of(rows[k + 1], base + PANEL)
            near = columns_of(rows[k + 1], base)
            rows[k + 1] = jnp.where(in_panel, 0.0, rows[k + 1])
        top = jnp.where(in_panel, jnp.where(col == row + base, 1.0, 0.0), rows[k])
        tops, scales, pairs = [], [], {}
        top_out = corner = jnp.zeros((PANEL, size), f32)
        for j in range(PANEL):
            scale = lax.rsqrt(over_sublanes(spread[j], j))
            scales.append(scale)
            lower = spread[j] * scale
            corner = jnp.where(col == base + j, lower, corner)
            top_row = over_sublanes(top, j) * scale
            tops.append(top_row)
            top_out = jnp.where(row == j, top_row, top_out)
            for c in range(j + 1, PANEL):
                pairs[j, c] = over_sublanes(spread[c], j) * scale
                spread[c] = spread[c] - lower * pairs[j, c]
            if j < PANEL - 1:
                top = top - lower * top_row
            if more:
                lower = near[j] * scale
                for c in range(j + 1, PANEL):
                    near[c] = near[c] - lower * pairs[j, c]
                for c in range(PANEL):
                    ahead[c] = ahead[c] - lower * over_sublanes(lower, c)
                rows[k + 1] = rows[k + 1] - lower * top_row
        upper_ref[base : base + PANEL, :] = jnp.where(col >= base + PANEL, top_out, 0.0)
        corner_ref[base : base + PANEL, :] = jnp.where(col <= row + base, corner, 0.0)
        inv_ref[base : base + PANEL, :] = jnp.where(col <= row + base, top_out, 0.0)
        if more:
            spread = ahead
        for i in range(k + 2, count):
            below = columns_of(rows[i], base)
            rows[i] = jnp.where(in_panel, 0.0, rows[i])
            for j in range(PANEL):
                lower = below[j] * scales[j]
                for c in range(j + 1, PANEL):
                    below[c] = below[c] - lower * pairs[j, c]
                rows[i] = rows[i] - lower * tops[j]


def cholesky_inverse(sym_ref, lower_ref, inv_ref, work_ref, tile_ref, corner_ref, unit_ref):
    width = sym_ref.shape[0]
    count = width // BLOCK
    work_ref[...] = sym_ref[:BLOCK, :BLOCK]

    def step(b, carry):
        factor_block(work_ref, tile_ref, corner_ref, unit_ref)
        for place in range(count):
            pl.when(b == place)(lambda place=place: after_block(place))
        return carry

    def after_block(b):
        lo, hi = b * BLOCK, (b + 1) * BLOCK
        unit = unit_ref[...]
        inv_ref[lo:hi, lo:hi] = unit
        lower_ref[lo:hi, lo:hi] = tile_ref[...].T + corner_ref[...]
        if hi < width:
            zero = jnp.zeros((BLOCK, width - hi), f32)
            lower_ref[lo:hi, hi:] = zero
            inv_ref[lo:hi, hi:] = zero
            below = dot_nt(sym_ref[hi:, lo:hi], unit)
            lower_ref[hi:, lo:hi] = below
            left = sym_ref[hi : hi + BLOCK, hi : hi + BLOCK] - dot_nt(below[:BLOCK], below[:BLOCK])
            work_ref[...] = mirror_lower(left)
            for j in range(b + 1, count):
                jlo, jhi = j * BLOCK, (j + 1) * BLOCK
                start = jhi if j == b + 1 else jlo
                if start < width:
                    sym_ref[start:, jlo:jhi] -= dot_nt(below[start - hi :], below[jlo - hi : jhi - hi])
        if b:
            inner = dot(lower_ref[lo:hi, :lo], inv_ref[:lo, :lo])
            inv_ref[lo:hi, :lo] = -dot(unit, inner)

    lax.fori_loop(0, count, step, 0)


def two_sum(left, right):
    total = left + right
    part = total - left
    return total, (left - (total - part)) + (right - part)


def exact_terms(value, triangular):
    anchor = jnp.max(jnp.abs(value), axis=1, keepdims=True) * (1.5 * 2.0**16)
    parts = []
    for k in range(SLICES):
        grid = jnp.broadcast_to(anchor * 2.0 ** (-8 * k), value.shape)
        part = (value + grid) - grid
        value = value - part
        parts.append(part.astype(jnp.bfloat16))
    for lo in range(0, value.shape[0], BLOCK):
        hi = lo + BLOCK
        inner = hi if triangular else value.shape[1]
        left = jnp.concatenate([part[lo:, :inner] for part in parts], axis=1)
        right = jnp.concatenate([part[lo:hi, :inner] for part in parts[::-1]], axis=1)
        terms = []
        for k in range(SLICES + 1):
            start, stop = max(0, k + 1 - SLICES) * inner, min(k + 1, SLICES) * inner
            back = max(0, SLICES - 1 - k) * inner
            terms.append(
                lax.dot_general(
                    left[:, start:stop],
                    right[:, back : back + stop - start],
                    (((1,), (1,)), ((), ())),
                    preferred_element_type=f32,
                )
            )
        yield terms


def halves(value):
    high = value.astype(jnp.bfloat16)
    return high, (value - high.astype(f32)).astype(jnp.bfloat16)


def dot3(left, right, left_dim=1, right_dim=0):
    lh, ll = halves(left)
    rh, rl = halves(right)
    return lax.dot_general(
        jnp.concatenate([lh, lh, ll], axis=left_dim),
        jnp.concatenate([rh, rl, rh], axis=right_dim),
        (((left_dim,), (right_dim,)), ((), ())),
        preferred_element_type=f32,
    )


def upper_times_lower(left, lower):
    size = lower.shape[0]
    out = []
    for lo in range(0, size, BLOCK):
        hi = lo + BLOCK
        column = dot3(left[:hi, lo:], lower[lo:, lo:hi])
        row, col = row_col(column.shape)
        column = jnp.where(row <= col + lo, column, 0.0)
        out.append(jnp.concatenate([column, jnp.zeros((size - hi, BLOCK), f32)], axis=0) if hi < size else column)
    return jnp.concatenate(out, axis=1)


def times_lower(left, lower):
    size = lower.shape[0]
    return jnp.concatenate(
        [dot3(left[:, lo:], lower[lo:, lo : lo + BLOCK]) for lo in range(0, size, BLOCK)], axis=1
    )


def lower_times_upper(lower, right):
    size = lower.shape[0]
    out = []
    for lo in range(0, size, BLOCK):
        hi = lo + BLOCK
        line = dot3(lower[lo:hi, :hi], right[:hi, lo:])
        row, col = row_col(line.shape)
        line = jnp.where(row <= col, line, 0.0)
        out.append(jnp.concatenate([jnp.zeros((BLOCK, lo), f32), line], axis=1) if lo else line)
    return jnp.concatenate(out, axis=0)


def lower_blocks(width):
    count = width // BLOCK
    return [(i, j) for j in range(count) for i in range(j, count)]


def upper_blocks(width):
    return [(j, i) for i, j in lower_blocks(width) if i > j]


def pieces_of(width):
    low = len(lower_blocks(width))
    return low, low + len(upper_blocks(width)), 2 * low + len(upper_blocks(width))


def span(block):
    return slice(block * BLOCK, (block + 1) * BLOCK)


def lo_lane(block):
    return slice(block * BLOCK, block * BLOCK + 1)


def gram_kernel(matrix_ref, grad_ref, out_ref):
    matrix, grad = matrix_ref[...], grad_ref[...]
    width = matrix.shape[1]
    count = width // BLOCK
    turned = matrix.T
    rows = BLOCK // CHUNKS
    row, col = row_col((BLOCK, BLOCK))
    lower, upper = lower_blocks(width), upper_blocks(width)
    low_at, upper_at = pieces_of(width)[1], pieces_of(width)[0]

    def put(piece, block):
        for c in range(CHUNKS):
            out_ref[c, piece] = block[c * rows : (c + 1) * rows, :]

    diag = jnp.sum(matrix * grad, axis=0, keepdims=True)
    crosses = [dot(turned[: (j + 1) * BLOCK], grad[:, span(j)]) for j in range(count)]
    for j, terms in enumerate(exact_terms(turned, False)):
        high, error = two_sum(terms[0], terms[1])
        low = error
        for term in terms[2:]:
            low = low + term
        total = high + low
        low = low - (total - high)
        for i in range(j, count):
            place = lower.index((i, j))
            here = slice((i - j) * BLOCK, (i - j + 1) * BLOCK)
            block, small = total[here], low[here]
            if i == j:
                block = jnp.where(row >= col, block, crosses[j][span(j)])
                first = jnp.broadcast_to(diag[:, lo_lane(j)], small.shape)
                small = jnp.where((row == 1) & (col == BLOCK - 1), first, small)
                small = jnp.where((row == 0) & (col > 0), jnp.broadcast_to(diag[:, span(j)], small.shape), small)
            put(place, block)
            put(low_at + place, small)
        for i in range(j):
            put(upper_at + upper.index((i, j)), crosses[j][span(i)])


def main_kernel(
    packed_ref, factor_hbm, matrix_hbm, grad_hbm, out_ref,
    sym_ref, cross_ref, lower1_ref, inv1_ref, lower2_ref, inv2_ref, full_ref, spread_ref, early_ref, factor_ref,
    work_ref, tile_ref, corner_ref, unit_ref, matrix_ref, grad_ref, before_ref, arrived, *, rate
):
    arrivals = [
        pltpu.make_async_copy(source, target, arrived.at[k])
        for k, (source, target) in enumerate(
            [(factor_hbm, factor_ref), (matrix_hbm, matrix_ref), (grad_hbm, grad_ref)]
        )
    ]
    for arrival in arrivals:
        arrival.start()
    width = matrix_ref.shape[1]
    count = width // BLOCK
    rows = BLOCK // CHUNKS
    row, col = row_col((BLOCK, BLOCK))
    on_diag = row == col
    lower, upper = lower_blocks(width), upper_blocks(width)
    upper_at, low_at, _ = pieces_of(width)

    def block_of(piece):
        return jnp.concatenate([packed_ref[c, piece] for c in range(CHUNKS)], axis=0)

    def trace_of(ref):
        total = jnp.zeros((1, 1), f32)
        for b in range(count):
            total += jnp.sum(jnp.where(on_diag, ref[span(b), span(b)], 0.0), keepdims=True)
        return total

    def shifted(block, shift):
        return block + jnp.where(on_diag, jnp.broadcast_to(shift, block.shape), 0.0)

    for place, (i, j) in enumerate(lower):
        block = block_of(place)
        if i == j:
            corner = packed_ref[0, low_at + place]
            diag = jnp.where(col[:1] == 0, corner[1:2, BLOCK - 1 :], corner[:1, :])
            diag = jnp.broadcast_to(diag, block.shape)
            cross_ref[span(i), span(i)] = jnp.where(row < col, block, jnp.where(on_diag, diag, 0.0))
            block = mirror_lower(block)
        else:
            cross_ref[span(i), span(j)] = jnp.zeros_like(block)
        sym_ref[span(i), span(j)] = block
    for place, (i, j) in enumerate(upper):
        cross_ref[span(i), span(j)] = block_of(upper_at + place)
    shift1 = trace_of(sym_ref) * rate
    for b in range(count):
        sym_ref[span(b), span(b)] = shifted(sym_ref[span(b), span(b)], shift1)
    cholesky_inverse(sym_ref, lower1_ref, inv1_ref, work_ref, tile_ref, corner_ref, unit_ref)

    for j, terms in enumerate(exact_terms(lower1_ref[...], True)):
        for i in range(j, count):
            place = lower.index((i, j))
            here = slice((i - j) * BLOCK, (i - j + 1) * BLOCK)
            high = block_of(place)
            rest = block_of(low_at + place)
            if i == j:
                high, error = two_sum(high, jnp.where(on_diag, jnp.broadcast_to(shift1, high.shape), 0.0))
                rest = rest + error
            high, error = two_sum(high, -terms[0][here])
            high, error2 = two_sum(high, -terms[1][here])
            rest = rest + (error + error2)
            for term in terms[2:]:
                rest = rest - term[here]
            block = high + rest
            if i == j:
                block = mirror_lower(block)
            else:
                full_ref[span(j), span(i)] = block.T
            full_ref[span(i), span(j)] = block
    inv1 = inv1_ref[...]
    spread = dot3(inv1, full_ref[...])
    for arrival in arrivals:
        arrival.wait()
    early_ref[...] = upper_times_lower(factor_ref[...], lower1_ref[...])
    before_ref[...] = dot_nt(matrix_ref[...], inv1)
    cross_ref[...] = dot(inv1, cross_ref[...])
    for j in range(count):
        lo = j * BLOCK
        spread_ref[lo:, span(j)] = dot_nt(inv1[lo:], inv1[span(j)])
        column = dot3(spread[lo:], inv1[span(j)], 1, 1) - jnp.broadcast_to(shift1, (width - lo, BLOCK)) * spread_ref[lo:, span(j)]
        for i in range(j, count):
            block = column[(i - j) * BLOCK : (i - j + 1) * BLOCK]
            if i == j:
                block = mirror_lower(jnp.where(on_diag, block + 1.0, block))
            else:
                full_ref[span(j), span(i)] = block.T
            full_ref[span(i), span(j)] = block
    shift2 = trace_of(full_ref) * rate
    for i, j in lower:
        block = full_ref[span(i), span(j)]
        sym_ref[span(i), span(j)] = shifted(block, shift2) if i == j else block
    cholesky_inverse(sym_ref, lower2_ref, inv2_ref, work_ref, tile_ref, corner_ref, unit_ref)

    inv1, inv2, lower1, lower2 = inv1_ref[...], inv2_ref[...], lower1_ref[...], lower2_ref[...]
    wide_row, wide_col = row_col((width, width))
    half = times_lower(cross_ref[...], inv2)
    second = early_ref[...] - lower_times_upper(inv2, half)
    middle = 0.5 * mirror_upper(upper_times_lower(second, lower2))
    side = times_lower(middle, inv2)
    weight = dot3(inv2, side, 0, 0) + jnp.where(wide_row == wide_col, rate * jnp.sum(side * inv2, keepdims=True), 0.0)
    crossed = half + 2.0 * dot3(full_ref[...], weight)
    first = lower_times_upper(lower2, factor_ref[...]) - upper_times_lower(crossed, inv1)
    middle = 0.5 * mirror_upper(upper_times_lower(first, lower1))
    trace = jnp.zeros((1, 1), f32)
    for i, j in lower:
        part = jnp.sum(middle[span(i), span(j)] * spread_ref[span(i), span(j)], keepdims=True)
        trace += part if i == j else 2.0 * part
    through = dot3(grad_ref[...], inv2) + 2.0 * dot3(before_ref[...], weight + middle)
    out_ref[...] = dot3(through, inv1) + (2.0 * rate) * trace * matrix_ref[...]


def exchange_levels(count):
    levels, stride = [], 1
    while stride < count:
        left = count // stride
        size = left if left <= 8 and levels else min(4, left)
        levels.append((stride, size))
        stride *= size
    return levels


def sum_over_devices(value, counts, low):
    rows_count, sub_count = counts
    levels = [("sub", 1, sub_count)] + [("rows", s, n) for s, n in exchange_levels(rows_count)]
    totals = {"rows": rows_count, "sub": sub_count}
    many, start = low

    def send(array, axis, change):
        return lax.ppermute(array, axis, [(i, i ^ change) for i in range(totals[axis])])

    def swap(mine, axis, stride):
        mine = lax.optimization_barrier(tuple(mine))
        return lax.optimization_barrier(
            (mine[0],) + tuple(send(mine[k], axis, k * stride) for k in range(1, len(mine)))
        )

    def add(left, right):
        total, error = two_sum(left, right)
        pad = [(0, 0)] * (total.ndim - 3) + [(start, 0), (0, 0), (0, 0)]
        return total + jnp.pad(error[..., :many, :, :], pad)

    def tree(values):
        while len(values) > 1:
            values = [add(values[i], values[i + 1]) for i in range(0, len(values), 2)]
        return values[0]

    split = []
    for axis, stride, size in levels:
        if value.shape[0] % size == 0:
            spot = (lax.axis_index(axis) // stride) % size
            pieces = value.reshape((size, value.shape[0] // size) + value.shape[1:])
            mine = [lax.dynamic_index_in_dim(pieces, spot ^ other, 0, False) for other in range(size)]
            split.append((axis, stride, size, spot))
            value = tree(swap(mine, axis, stride))
        else:
            change = 1
            while change < size:
                value = add(value, send(value, axis, change * stride))
                change = 2 * change + 1
    for axis, stride, size, spot in split[::-1]:
        got = swap([value] * size, axis, stride)
        pieces = jnp.zeros((size,) + value.shape, f32)
        for other in range(size):
            pieces = lax.dynamic_update_index_in_dim(pieces, got[other], spot ^ other, 0)
        value = pieces.reshape((size * value.shape[0],) + value.shape[1:])
    return value


def call(kernel, out_shapes, scratch_shapes, *operands, spaces=None):
    vmem = pl.BlockSpec(memory_space=pltpu.VMEM)
    return pl.pallas_call(
        kernel,
        out_shape=out_shapes,
        in_specs=spaces or [vmem] * len(operands),
        out_specs=[vmem] * len(out_shapes),
        scratch_shapes=scratch_shapes,
    )(*operands)


def run_gram(matrix, grad_out):
    shape = (CHUNKS, pieces_of(matrix.shape[1])[2], BLOCK // CHUNKS, BLOCK)
    return call(gram_kernel, [pltpu.VMEM(shape, f32)], [], matrix, grad_out)[0]


def run_main(packed, grad_factor, matrix, grad_out):
    width = matrix.shape[1]
    square, tile, rows = [pltpu.VMEM(s, f32) for s in ((width, width), (BLOCK, BLOCK), matrix.shape)]

    def main(*refs):
        main_kernel(*refs, rate=shift_frac / width)

    packed = pltpu.with_memory_space_constraint(packed, pltpu.VMEM)
    scratch = [square] * 10 + [tile] * 4 + [rows] * 3 + [pltpu.SemaphoreType.DMA((3,))]
    spaces = [pl.BlockSpec(memory_space=pltpu.VMEM)] + [pl.BlockSpec(memory_space=pl.ANY)] * 3
    out = jax.ShapeDtypeStruct(matrix.shape, f32)
    return call(main, [out], scratch, packed, grad_factor, matrix, grad_out, spaces=spaces)[0]


def solution(mesh):
    counts = (mesh.shape["rows"], mesh.shape["sub"])

    def per_device(matrix, grad_out, grad_factor):
        many, start, _ = pieces_of(matrix.shape[1])
        packed = sum_over_devices(run_gram(matrix, grad_out), counts, (many, start))
        return run_main(packed, grad_factor, matrix, grad_out)

    placed = (P(("rows", "sub"), None), P(("rows", "sub"), None), P())
    return jax.shard_map(
        per_device, mesh=mesh, in_specs=placed, out_specs=P(("rows", "sub"), None), check_vma=False
    )
```

```python
import jax
import jax.numpy as jnp
from jax import lax
from jax.experimental import pallas as pl
from jax.experimental.pallas import tpu as pltpu
from jax.sharding import PartitionSpec as P

SECTIONS = 2
BLOCK = 128
PANEL = 8
CHUNKS = 8
SLICES = 4

shift_frac = 0.02


f32 = jnp.float32


def thirds(value):
    high = value.astype(jnp.bfloat16)
    value = value - high.astype(f32)
    middle = value.astype(jnp.bfloat16)
    return high, middle, (value - middle.astype(f32)).astype(jnp.bfloat16)


def dot(left, right, left_dim=1, right_dim=0):
    lh, lm, ll = thirds(left)
    rh, rm, rl = thirds(right)

    def side_by_side(lefts, rights):
        return lax.dot_general(
            jnp.concatenate(lefts, axis=left_dim),
            jnp.concatenate(rights, axis=right_dim),
            (((left_dim,), (right_dim,)), ((), ())),
            preferred_element_type=f32,
        )

    return side_by_side([lh, lm, lh, ll], [rl, rm, rm, rh]) + side_by_side([lm, lh], [rh, rh])


def dot_nt(left, right):
    return dot(left, right, 1, 1)


def row_col(shape):
    return lax.broadcasted_iota(jnp.int32, shape, 0), lax.broadcasted_iota(jnp.int32, shape, 1)


def mirror_lower(block):
    row, col = row_col(block.shape)
    return jnp.where(row >= col, block, block.T)


def mirror_upper(block):
    row, col = row_col(block.shape)
    return jnp.where(row <= col, block, block.T)


def factor_block(sym_ref, upper_ref, corner_ref, inv_ref):
    size = sym_ref.shape[0]
    count = size // PANEL
    row, col = row_col((PANEL, size))
    rows = [sym_ref[PANEL * i : PANEL * (i + 1), :] for i in range(count)]

    def over_lanes(value, lane):
        return jnp.broadcast_to(value[:, lane : lane + 1], (PANEL, size))

    def over_sublanes(value, sublane):
        return jnp.broadcast_to(value[sublane : sublane + 1, :], (PANEL, size))

    def columns_of(value, base):
        return [over_lanes(value, base + c) for c in range(PANEL)]

    spread = columns_of(rows[0], 0)
    for k in range(count):
        base = PANEL * k
        more = k + 1 < count
        in_panel = (col >= base) & (col < base + PANEL)
        if more:
            ahead = columns_of(rows[k + 1], base + PANEL)
            near = columns_of(rows[k + 1], base)
            rows[k + 1] = jnp.where(in_panel, 0.0, rows[k + 1])
        top = jnp.where(in_panel, jnp.where(col == row + base, 1.0, 0.0), rows[k])
        tops, scales, pairs = [], [], {}
        top_out = corner = jnp.zeros((PANEL, size), f32)
        for j in range(PANEL):
            scale = lax.rsqrt(over_sublanes(spread[j], j))
            scales.append(scale)
            lower = spread[j] * scale
            corner = jnp.where(col == base + j, lower, corner)
            top_row = over_sublanes(top, j) * scale
            tops.append(top_row)
            top_out = jnp.where(row == j, top_row, top_out)
            for c in range(j + 1, PANEL):
                pairs[j, c] = over_sublanes(spread[c], j) * scale
                spread[c] = spread[c] - lower * pairs[j, c]
            if j < PANEL - 1:
                top = top - lower * top_row
            if more:
                lower = near[j] * scale
                for c in range(j + 1, PANEL):
                    near[c] = near[c] - lower * pairs[j, c]
                for c in range(PANEL):
                    ahead[c] = ahead[c] - lower * over_sublanes(lower, c)
                rows[k + 1] = rows[k + 1] - lower * top_row
        upper_ref[base : base + PANEL, :] = jnp.where(col >= base + PANEL, top_out, 0.0)
        corner_ref[base : base + PANEL, :] = jnp.where(col <= row + base, corner, 0.0)
        inv_ref[base : base + PANEL, :] = jnp.where(col <= row + base, top_out, 0.0)
        if more:
            spread = ahead
        for i in range(k + 2, count):
            below = columns_of(rows[i], base)
            rows[i] = jnp.where(in_panel, 0.0, rows[i])
            for j in range(PANEL):
                lower = below[j] * scales[j]
                for c in range(j + 1, PANEL):
                    below[c] = below[c] - lower * pairs[j, c]
                rows[i] = rows[i] - lower * tops[j]


def cholesky_inverse(sym_ref, lower_ref, inv_ref, work_ref, tile_ref, corner_ref, unit_ref):
    width = sym_ref.shape[0]
    count = width // BLOCK
    work_ref[...] = sym_ref[:BLOCK, :BLOCK]

    def step(b, carry):
        factor_block(work_ref, tile_ref, corner_ref, unit_ref)
        for place in range(count):
            pl.when(b == place)(lambda place=place: after_block(place))
        return carry

    def after_block(b):
        lo, hi = b * BLOCK, (b + 1) * BLOCK
        unit = unit_ref[...]
        inv_ref[lo:hi, lo:hi] = unit
        lower_ref[lo:hi, lo:hi] = tile_ref[...].T + corner_ref[...]
        if hi < width:
            zero = jnp.zeros((BLOCK, width - hi), f32)
            lower_ref[lo:hi, hi:] = zero
            inv_ref[lo:hi, hi:] = zero
            below = dot_nt(sym_ref[hi:, lo:hi], unit)
            lower_ref[hi:, lo:hi] = below
            left = sym_ref[hi : hi + BLOCK, hi : hi + BLOCK] - dot_nt(below[:BLOCK], below[:BLOCK])
            work_ref[...] = mirror_lower(left)
            for j in range(b + 1, count):
                jlo, jhi = j * BLOCK, (j + 1) * BLOCK
                start = jhi if j == b + 1 else jlo
                if start < width:
                    sym_ref[start:, jlo:jhi] -= dot_nt(below[start - hi :], below[jlo - hi : jhi - hi])
        if b:
            inner = dot(lower_ref[lo:hi, :lo], inv_ref[:lo, :lo])
            inv_ref[lo:hi, :lo] = -dot(unit, inner)

    lax.fori_loop(0, count, step, 0)


def two_sum(left, right):
    total = left + right
    part = total - left
    return total, (left - (total - part)) + (right - part)


def exact_terms(value, triangular):
    anchor = jnp.max(jnp.abs(value), axis=1, keepdims=True) * (1.5 * 2.0**16)
    parts = []
    for k in range(SLICES):
        grid = jnp.broadcast_to(anchor * 2.0 ** (-8 * k), value.shape)
        part = (value + grid) - grid
        value = value - part
        parts.append(part.astype(jnp.bfloat16))
    for lo in range(0, value.shape[0], BLOCK):
        hi = lo + BLOCK
        inner = hi if triangular else value.shape[1]
        left = jnp.concatenate([part[lo:, :inner] for part in parts], axis=1)
        right = jnp.concatenate([part[lo:hi, :inner] for part in parts[::-1]], axis=1)
        terms = []
        for k in range(SLICES + 1):
            start, stop = max(0, k + 1 - SLICES) * inner, min(k + 1, SLICES) * inner
            back = max(0, SLICES - 1 - k) * inner
            terms.append(
                lax.dot_general(
                    left[:, start:stop],
                    right[:, back : back + stop - start],
                    (((1,), (1,)), ((), ())),
                    preferred_element_type=f32,
                )
            )
        yield terms


def halves(value):
    high = value.astype(jnp.bfloat16)
    return high, (value - high.astype(f32)).astype(jnp.bfloat16)


def dot3(left, right, left_dim=1, right_dim=0):
    lh, ll = halves(left)
    rh, rl = halves(right)
    return lax.dot_general(
        jnp.concatenate([lh, lh, ll], axis=left_dim),
        jnp.concatenate([rh, rl, rh], axis=right_dim),
        (((left_dim,), (right_dim,)), ((), ())),
        preferred_element_type=f32,
    )


def upper_times_lower(left, lower):
    size = lower.shape[0]
    out = []
    for lo in range(0, size, BLOCK):
        hi = lo + BLOCK
        column = dot3(left[:hi, lo:], lower[lo:, lo:hi])
        row, col = row_col(column.shape)
        column = jnp.where(row <= col + lo, column, 0.0)
        out.append(jnp.concatenate([column, jnp.zeros((size - hi, BLOCK), f32)], axis=0) if hi < size else column)
    return jnp.concatenate(out, axis=1)


def times_lower(left, lower):
    size = lower.shape[0]
    return jnp.concatenate(
        [dot3(left[:, lo:], lower[lo:, lo : lo + BLOCK]) for lo in range(0, size, BLOCK)], axis=1
    )


def lower_times_upper(lower, right):
    size = lower.shape[0]
    out = []
    for lo in range(0, size, BLOCK):
        hi = lo + BLOCK
        line = dot3(lower[lo:hi, :hi], right[:hi, lo:])
        row, col = row_col(line.shape)
        line = jnp.where(row <= col, line, 0.0)
        out.append(jnp.concatenate([jnp.zeros((BLOCK, lo), f32), line], axis=1) if lo else line)
    return jnp.concatenate(out, axis=0)


def lower_blocks(width):
    count = width // BLOCK
    return [(i, j) for j in range(count) for i in range(j, count)]


def upper_blocks(width):
    return [(j, i) for i, j in lower_blocks(width) if i > j]


def pieces_of(width):
    low = len(lower_blocks(width))
    return low, low + len(upper_blocks(width)), 2 * low + len(upper_blocks(width))


def span(block):
    return slice(block * BLOCK, (block + 1) * BLOCK)


def lo_lane(block):
    return slice(block * BLOCK, block * BLOCK + 1)


def gram_kernel(matrix_ref, grad_ref, out_ref):
    matrix, grad = matrix_ref[...], grad_ref[...]
    width = matrix.shape[1]
    count = width // BLOCK
    turned = matrix.T
    rows = BLOCK // CHUNKS
    row, col = row_col((BLOCK, BLOCK))
    lower, upper = lower_blocks(width), upper_blocks(width)
    low_at, upper_at = pieces_of(width)[1], pieces_of(width)[0]

    def put(piece, block):
        for c in range(CHUNKS):
            out_ref[c, piece] = block[c * rows : (c + 1) * rows, :]

    diag = jnp.sum(matrix * grad, axis=0, keepdims=True)
    crosses = [dot(turned[: (j + 1) * BLOCK], grad[:, span(j)]) for j in range(count)]
    for j, terms in enumerate(exact_terms(turned, False)):
        high, error = two_sum(terms[0], terms[1])
        low = error
        for term in terms[2:]:
            low = low + term
        total = high + low
        low = low - (total - high)
        for i in range(j, count):
            place = lower.index((i, j))
            here = slice((i - j) * BLOCK, (i - j + 1) * BLOCK)
            block, small = total[here], low[here]
            if i == j:
                block = jnp.where(row >= col, block, crosses[j][span(j)])
                first = jnp.broadcast_to(diag[:, lo_lane(j)], small.shape)
                small = jnp.where((row == 1) & (col == BLOCK - 1), first, small)
                small = jnp.where((row == 0) & (col > 0), jnp.broadcast_to(diag[:, span(j)], small.shape), small)
            put(place, block)
            put(low_at + place, small)
        for i in range(j):
            put(upper_at + upper.index((i, j)), crosses[j][span(i)])


def main_kernel(
    packed_ref, factor_hbm, matrix_hbm, grad_hbm, out_ref,
    sym_ref, cross_ref, lower1_ref, inv1_ref, lower2_ref, inv2_ref, full_ref, spread_ref, early_ref, factor_ref,
    work_ref, tile_ref, corner_ref, unit_ref, matrix_ref, grad_ref, before_ref, arrived, *, rate
):
    arrivals = [
        pltpu.make_async_copy(source, target, arrived.at[k])
        for k, (source, target) in enumerate(
            [(factor_hbm, factor_ref), (matrix_hbm, matrix_ref), (grad_hbm, grad_ref)]
        )
    ]
    for arrival in arrivals:
        arrival.start()
    width = matrix_ref.shape[1]
    count = width // BLOCK
    rows = BLOCK // CHUNKS
    row, col = row_col((BLOCK, BLOCK))
    on_diag = row == col
    lower, upper = lower_blocks(width), upper_blocks(width)
    upper_at, low_at, _ = pieces_of(width)

    def block_of(piece):
        return jnp.concatenate([packed_ref[c, piece] for c in range(CHUNKS)], axis=0)

    def trace_of(ref):
        total = jnp.zeros((1, 1), f32)
        for b in range(count):
            total += jnp.sum(jnp.where(on_diag, ref[span(b), span(b)], 0.0), keepdims=True)
        return total

    def shifted(block, shift):
        return block + jnp.where(on_diag, jnp.broadcast_to(shift, block.shape), 0.0)

    for place, (i, j) in enumerate(lower):
        block = block_of(place)
        if i == j:
            corner = packed_ref[0, low_at + place]
            diag = jnp.where(col[:1] == 0, corner[1:2, BLOCK - 1 :], corner[:1, :])
            diag = jnp.broadcast_to(diag, block.shape)
            cross_ref[span(i), span(i)] = jnp.where(row < col, block, jnp.where(on_diag, diag, 0.0))
            block = mirror_lower(block)
        else:
            cross_ref[span(i), span(j)] = jnp.zeros_like(block)
        sym_ref[span(i), span(j)] = block
    for place, (i, j) in enumerate(upper):
        cross_ref[span(i), span(j)] = block_of(upper_at + place)
    shift1 = trace_of(sym_ref) * rate
    for b in range(count):
        sym_ref[span(b), span(b)] = shifted(sym_ref[span(b), span(b)], shift1)
    cholesky_inverse(sym_ref, lower1_ref, inv1_ref, work_ref, tile_ref, corner_ref, unit_ref)

    for j, terms in enumerate(exact_terms(lower1_ref[...], True)):
        for i in range(j, count):
            place = lower.index((i, j))
            here = slice((i - j) * BLOCK, (i - j + 1) * BLOCK)
            high = block_of(place)
            rest = block_of(low_at + place)
            if i == j:
                high, error = two_sum(high, jnp.where(on_diag, jnp.broadcast_to(shift1, high.shape), 0.0))
                rest = rest + error
            high, error = two_sum(high, -terms[0][here])
            high, error2 = two_sum(high, -terms[1][here])
            rest = rest + (error + error2)
            for term in terms[2:]:
                rest = rest - term[here]
            block = high + rest
            if i == j:
                block = mirror_lower(block)
            else:
                full_ref[span(j), span(i)] = block.T
            full_ref[span(i), span(j)] = block
    inv1 = inv1_ref[...]
    spread = dot3(inv1, full_ref[...])
    for arrival in arrivals:
        arrival.wait()
    early_ref[...] = upper_times_lower(factor_ref[...], lower1_ref[...])
    before_ref[...] = dot_nt(matrix_ref[...], inv1)
    cross_ref[...] = dot(inv1, cross_ref[...])
    for j in range(count):
        lo = j * BLOCK
        hi = lo + BLOCK
        spread_ref[lo:, span(j)] = dot_nt(inv1[lo:, :hi], inv1[span(j), :hi])
        column = dot3(spread[lo:, :hi], inv1[span(j), :hi], 1, 1)
        column -= jnp.broadcast_to(shift1, (width - lo, BLOCK)) * spread_ref[lo:, span(j)]
        for i in range(j, count):
            block = column[(i - j) * BLOCK : (i - j + 1) * BLOCK]
            if i == j:
                block = mirror_lower(jnp.where(on_diag, block + 1.0, block))
            else:
                full_ref[span(j), span(i)] = block.T
            full_ref[span(i), span(j)] = block
    shift2 = trace_of(full_ref) * rate
    for i, j in lower:
        block = full_ref[span(i), span(j)]
        sym_ref[span(i), span(j)] = shifted(block, shift2) if i == j else block
    cholesky_inverse(sym_ref, lower2_ref, inv2_ref, work_ref, tile_ref, corner_ref, unit_ref)

    inv1, inv2, lower1, lower2 = inv1_ref[...], inv2_ref[...], lower1_ref[...], lower2_ref[...]
    wide_row, wide_col = row_col((width, width))
    half = times_lower(cross_ref[...], inv2)
    second = early_ref[...] - lower_times_upper(inv2, half)
    middle = 0.5 * mirror_upper(upper_times_lower(second, lower2))
    side = times_lower(middle, inv2)
    weight = dot3(inv2, side, 0, 0) + jnp.where(wide_row == wide_col, rate * jnp.sum(side * inv2, keepdims=True), 0.0)
    crossed = half + 2.0 * dot3(full_ref[...], weight)
    first = lower_times_upper(lower2, factor_ref[...]) - upper_times_lower(crossed, inv1)
    middle = 0.5 * mirror_upper(upper_times_lower(first, lower1))
    trace = jnp.zeros((1, 1), f32)
    for i, j in lower:
        part = jnp.sum(middle[span(i), span(j)] * spread_ref[span(i), span(j)], keepdims=True)
        trace += part if i == j else 2.0 * part
    through = dot3(grad_ref[...], inv2) + 2.0 * dot3(before_ref[...], weight + middle)
    out_ref[...] = dot3(through, inv1) + (2.0 * rate) * trace * matrix_ref[...]


def exchange_levels(count):
    levels, stride = [], 1
    while stride < count:
        left = count // stride
        size = left if left <= 8 and levels else min(4, left)
        levels.append((stride, size))
        stride *= size
    return levels


def sum_over_devices(value, counts, low):
    rows_count, sub_count = counts
    levels = [("sub", 1, sub_count)] + [("rows", s, n) for s, n in exchange_levels(rows_count)]
    totals = {"rows": rows_count, "sub": sub_count}
    many, start = low

    def send(array, axis, change):
        return lax.ppermute(array, axis, [(i, i ^ change) for i in range(totals[axis])])

    def swap(mine, axis, stride):
        mine = lax.optimization_barrier(tuple(mine))
        return lax.optimization_barrier(
            (mine[0],) + tuple(send(mine[k], axis, k * stride) for k in range(1, len(mine)))
        )

    def add(left, right):
        total, error = two_sum(left, right)
        pad = [(0, 0)] * (total.ndim - 3) + [(start, 0), (0, 0), (0, 0)]
        return total + jnp.pad(error[..., :many, :, :], pad)

    def tree(values):
        while len(values) > 1:
            values = [add(values[i], values[i + 1]) for i in range(0, len(values), 2)]
        return values[0]

    split = []
    for axis, stride, size in levels:
        if value.shape[0] % size == 0:
            spot = (lax.axis_index(axis) // stride) % size
            pieces = value.reshape((size, value.shape[0] // size) + value.shape[1:])
            mine = [lax.dynamic_index_in_dim(pieces, spot ^ other, 0, False) for other in range(size)]
            split.append((axis, stride, size, spot))
            value = tree(swap(mine, axis, stride))
        else:
            change = 1
            while change < size:
                value = add(value, send(value, axis, change * stride))
                change = 2 * change + 1
    for axis, stride, size, spot in split[::-1]:
        got = swap([value] * size, axis, stride)
        pieces = jnp.zeros((size,) + value.shape, f32)
        for other in range(size):
            pieces = lax.dynamic_update_index_in_dim(pieces, got[other], spot ^ other, 0)
        value = pieces.reshape((size * value.shape[0],) + value.shape[1:])
    return value


def call(kernel, out_shapes, scratch_shapes, *operands, spaces=None):
    vmem = pl.BlockSpec(memory_space=pltpu.VMEM)
    return pl.pallas_call(
        kernel,
        out_shape=out_shapes,
        in_specs=spaces or [vmem] * len(operands),
        out_specs=[vmem] * len(out_shapes),
        scratch_shapes=scratch_shapes,
    )(*operands)


def run_gram(matrix, grad_out):
    shape = (CHUNKS, pieces_of(matrix.shape[1])[2], BLOCK // CHUNKS, BLOCK)
    return call(gram_kernel, [pltpu.VMEM(shape, f32)], [], matrix, grad_out)[0]


def run_main(packed, grad_factor, matrix, grad_out):
    width = matrix.shape[1]
    square, tile, rows = [pltpu.VMEM(s, f32) for s in ((width, width), (BLOCK, BLOCK), matrix.shape)]

    def main(*refs):
        main_kernel(*refs, rate=shift_frac / width)

    packed = pltpu.with_memory_space_constraint(packed, pltpu.VMEM)
    scratch = [square] * 10 + [tile] * 4 + [rows] * 3 + [pltpu.SemaphoreType.DMA((3,))]
    spaces = [pl.BlockSpec(memory_space=pltpu.VMEM)] + [pl.BlockSpec(memory_space=pl.ANY)] * 3
    out = jax.ShapeDtypeStruct(matrix.shape, f32)
    return call(main, [out], scratch, packed, grad_factor, matrix, grad_out, spaces=spaces)[0]


def solution(mesh):
    counts = (mesh.shape["rows"], mesh.shape["sub"])

    def per_device(matrix, grad_out, grad_factor):
        many, start, _ = pieces_of(matrix.shape[1])
        packed = sum_over_devices(run_gram(matrix, grad_out), counts, (many, start))
        return run_main(packed, grad_factor, matrix, grad_out)

    placed = (P(("rows", "sub"), None), P(("rows", "sub"), None), P())
    return jax.shard_map(
        per_device, mesh=mesh, in_specs=placed, out_specs=P(("rows", "sub"), None), check_vma=False
    )
```

```python
import jax
import jax.numpy as jnp
from jax import lax
from jax.experimental import pallas as pl
from jax.experimental.pallas import tpu as pltpu
from jax.sharding import PartitionSpec as P

SECTIONS = 2
BLOCK = 128
PANEL = 8
CHUNKS = 8
SLICES = 4

shift_frac = 0.02


f32 = jnp.float32


def thirds(value):
    high = value.astype(jnp.bfloat16)
    value = value - high.astype(f32)
    middle = value.astype(jnp.bfloat16)
    return high, middle, (value - middle.astype(f32)).astype(jnp.bfloat16)


def dot(left, right, left_dim=1, right_dim=0):
    lh, lm, ll = thirds(left)
    rh, rm, rl = thirds(right)

    def side_by_side(lefts, rights):
        return lax.dot_general(
            jnp.concatenate(lefts, axis=left_dim),
            jnp.concatenate(rights, axis=right_dim),
            (((left_dim,), (right_dim,)), ((), ())),
            preferred_element_type=f32,
        )

    return side_by_side([lh, lm, lh, ll], [rl, rm, rm, rh]) + side_by_side([lm, lh], [rh, rh])


def dot_nt(left, right):
    return dot(left, right, 1, 1)


def row_col(shape):
    return lax.broadcasted_iota(jnp.int32, shape, 0), lax.broadcasted_iota(jnp.int32, shape, 1)


def mirror_lower(block):
    row, col = row_col(block.shape)
    return jnp.where(row >= col, block, block.T)


def mirror_upper(block):
    row, col = row_col(block.shape)
    return jnp.where(row <= col, block, block.T)


def factor_block(sym_ref, upper_ref, corner_ref, inv_ref):
    size = sym_ref.shape[0]
    count = size // PANEL
    row, col = row_col((PANEL, size))
    rows = [sym_ref[PANEL * i : PANEL * (i + 1), :] for i in range(count)]

    def over_lanes(value, lane):
        return jnp.broadcast_to(value[:, lane : lane + 1], (PANEL, size))

    def over_sublanes(value, sublane):
        return jnp.broadcast_to(value[sublane : sublane + 1, :], (PANEL, size))

    def columns_of(value, base):
        return [over_lanes(value, base + c) for c in range(PANEL)]

    spread = columns_of(rows[0], 0)
    for k in range(count):
        base = PANEL * k
        more = k + 1 < count
        in_panel = (col >= base) & (col < base + PANEL)
        if more:
            ahead = columns_of(rows[k + 1], base + PANEL)
            near = columns_of(rows[k + 1], base)
            rows[k + 1] = jnp.where(in_panel, 0.0, rows[k + 1])
        top = jnp.where(in_panel, jnp.where(col == row + base, 1.0, 0.0), rows[k])
        tops, scales, pairs = [], [], {}
        top_out = corner = jnp.zeros((PANEL, size), f32)
        for j in range(PANEL):
            scale = lax.rsqrt(over_sublanes(spread[j], j))
            scales.append(scale)
            lower = spread[j] * scale
            corner = jnp.where(col == base + j, lower, corner)
            top_row = over_sublanes(top, j) * scale
            tops.append(top_row)
            top_out = jnp.where(row == j, top_row, top_out)
            for c in range(j + 1, PANEL):
                pairs[j, c] = over_sublanes(spread[c], j) * scale
                spread[c] = spread[c] - lower * pairs[j, c]
            if j < PANEL - 1:
                top = top - lower * top_row
            if more:
                lower = near[j] * scale
                for c in range(j + 1, PANEL):
                    near[c] = near[c] - lower * pairs[j, c]
                for c in range(PANEL):
                    ahead[c] = ahead[c] - lower * over_sublanes(lower, c)
                rows[k + 1] = rows[k + 1] - lower * top_row
        upper_ref[base : base + PANEL, :] = jnp.where(col >= base + PANEL, top_out, 0.0)
        corner_ref[base : base + PANEL, :] = jnp.where(col <= row + base, corner, 0.0)
        inv_ref[base : base + PANEL, :] = jnp.where(col <= row + base, top_out, 0.0)
        if more:
            spread = ahead
        for i in range(k + 2, count):
            below = columns_of(rows[i], base)
            rows[i] = jnp.where(in_panel, 0.0, rows[i])
            for j in range(PANEL):
                lower = below[j] * scales[j]
                for c in range(j + 1, PANEL):
                    below[c] = below[c] - lower * pairs[j, c]
                rows[i] = rows[i] - lower * tops[j]


def cholesky_inverse(sym_ref, lower_ref, inv_ref, work_ref, tile_ref, corner_ref, unit_ref):
    width = sym_ref.shape[0]
    count = width // BLOCK
    work_ref[...] = sym_ref[:BLOCK, :BLOCK]

    def step(b, carry):
        factor_block(work_ref, tile_ref, corner_ref, unit_ref)
        for place in range(count):
            pl.when(b == place)(lambda place=place: after_block(place))
        return carry

    def after_block(b):
        lo, hi = b * BLOCK, (b + 1) * BLOCK
        unit = unit_ref[...]
        inv_ref[lo:hi, lo:hi] = unit
        lower_ref[lo:hi, lo:hi] = tile_ref[...].T + corner_ref[...]
        if hi < width:
            zero = jnp.zeros((BLOCK, width - hi), f32)
            lower_ref[lo:hi, hi:] = zero
            inv_ref[lo:hi, hi:] = zero
            below = dot_nt(sym_ref[hi:, lo:hi], unit)
            lower_ref[hi:, lo:hi] = below
            left = sym_ref[hi : hi + BLOCK, hi : hi + BLOCK] - dot_nt(below[:BLOCK], below[:BLOCK])
            work_ref[...] = mirror_lower(left)
            for j in range(b + 1, count):
                jlo, jhi = j * BLOCK, (j + 1) * BLOCK
                start = jhi if j == b + 1 else jlo
                if start < width:
                    sym_ref[start:, jlo:jhi] -= dot_nt(below[start - hi :], below[jlo - hi : jhi - hi])
        if b:
            inner = dot(lower_ref[lo:hi, :lo], inv_ref[:lo, :lo])
            inv_ref[lo:hi, :lo] = -dot(unit, inner)

    lax.fori_loop(0, count, step, 0)


def two_sum(left, right):
    total = left + right
    part = total - left
    return total, (left - (total - part)) + (right - part)


def exact_terms(value, triangular):
    anchor = jnp.max(jnp.abs(value), axis=1, keepdims=True) * (1.5 * 2.0**16)
    parts = []
    for k in range(SLICES):
        grid = jnp.broadcast_to(anchor * 2.0 ** (-8 * k), value.shape)
        part = (value + grid) - grid
        value = value - part
        parts.append(part.astype(jnp.bfloat16))
    for lo in range(0, value.shape[0], BLOCK):
        hi = lo + BLOCK
        inner = hi if triangular else value.shape[1]
        left = jnp.concatenate([part[lo:, :inner] for part in parts], axis=1)
        right = jnp.concatenate([part[lo:hi, :inner] for part in parts[::-1]], axis=1)
        terms = []
        for k in range(SLICES + 1):
            start, stop = max(0, k + 1 - SLICES) * inner, min(k + 1, SLICES) * inner
            back = max(0, SLICES - 1 - k) * inner
            terms.append(
                lax.dot_general(
                    left[:, start:stop],
                    right[:, back : back + stop - start],
                    (((1,), (1,)), ((), ())),
                    preferred_element_type=f32,
                )
            )
        yield terms


def halves(value):
    high = value.astype(jnp.bfloat16)
    return high, (value - high.astype(f32)).astype(jnp.bfloat16)


def dot3(left, right, left_dim=1, right_dim=0):
    lh, ll = halves(left)
    rh, rl = halves(right)
    return lax.dot_general(
        jnp.concatenate([lh, lh, ll], axis=left_dim),
        jnp.concatenate([rh, rl, rh], axis=right_dim),
        (((left_dim,), (right_dim,)), ((), ())),
        preferred_element_type=f32,
    )


def upper_times_lower(left, lower):
    size = lower.shape[0]
    out = []
    for lo in range(0, size, BLOCK):
        hi = lo + BLOCK
        column = dot3(left[:hi, lo:], lower[lo:, lo:hi])
        row, col = row_col(column.shape)
        column = jnp.where(row <= col + lo, column, 0.0)
        out.append(jnp.concatenate([column, jnp.zeros((size - hi, BLOCK), f32)], axis=0) if hi < size else column)
    return jnp.concatenate(out, axis=1)


def times_lower(left, lower):
    size = lower.shape[0]
    return jnp.concatenate(
        [dot3(left[:, lo:], lower[lo:, lo : lo + BLOCK]) for lo in range(0, size, BLOCK)], axis=1
    )


def lower_times_upper(lower, right):
    size = lower.shape[0]
    out = []
    for lo in range(0, size, BLOCK):
        hi = lo + BLOCK
        line = dot3(lower[lo:hi, :hi], right[:hi, lo:])
        row, col = row_col(line.shape)
        line = jnp.where(row <= col, line, 0.0)
        out.append(jnp.concatenate([jnp.zeros((BLOCK, lo), f32), line], axis=1) if lo else line)
    return jnp.concatenate(out, axis=0)


def lower_blocks(width):
    count = width // BLOCK
    return [(i, j) for j in range(count) for i in range(j, count)]


def upper_blocks(width):
    return [(j, i) for i, j in lower_blocks(width) if i > j]


def pieces_of(width):
    low = len(lower_blocks(width))
    return low, low + len(upper_blocks(width)), 2 * low + len(upper_blocks(width))


def span(block):
    return slice(block * BLOCK, (block + 1) * BLOCK)


def lo_lane(block):
    return slice(block * BLOCK, block * BLOCK + 1)


def gram_kernel(matrix_ref, grad_ref, out_ref):
    matrix, grad = matrix_ref[...], grad_ref[...]
    width = matrix.shape[1]
    count = width // BLOCK
    turned = matrix.T
    rows = BLOCK // CHUNKS
    row, col = row_col((BLOCK, BLOCK))
    lower, upper = lower_blocks(width), upper_blocks(width)
    low_at, upper_at = pieces_of(width)[1], pieces_of(width)[0]

    def put(piece, block):
        for c in range(CHUNKS):
            out_ref[c, piece] = block[c * rows : (c + 1) * rows, :]

    diag = jnp.sum(matrix * grad, axis=0, keepdims=True)
    crosses = [dot(turned[: (j + 1) * BLOCK], grad[:, span(j)]) for j in range(count)]
    for j, terms in enumerate(exact_terms(turned, False)):
        high, error = two_sum(terms[0], terms[1])
        low = error
        for term in terms[2:]:
            low = low + term
        total = high + low
        low = low - (total - high)
        for i in range(j, count):
            place = lower.index((i, j))
            here = slice((i - j) * BLOCK, (i - j + 1) * BLOCK)
            block, small = total[here], low[here]
            if i == j:
                block = jnp.where(row >= col, block, crosses[j][span(j)])
                first = jnp.broadcast_to(diag[:, lo_lane(j)], small.shape)
                small = jnp.where((row == 1) & (col == BLOCK - 1), first, small)
                small = jnp.where((row == 0) & (col > 0), jnp.broadcast_to(diag[:, span(j)], small.shape), small)
            put(place, block)
            put(low_at + place, small)
        for i in range(j):
            put(upper_at + upper.index((i, j)), crosses[j][span(i)])


def main_kernel(
    packed_ref, factor_hbm, matrix_hbm, grad_hbm, out_ref,
    sym_ref, cross_ref, lower1_ref, inv1_ref, lower2_ref, inv2_ref, full_ref, spread_ref, early_ref, factor_ref,
    work_ref, tile_ref, corner_ref, unit_ref, matrix_ref, grad_ref, before_ref, arrived, *, rate
):
    arrivals = [
        pltpu.make_async_copy(source, target, arrived.at[k])
        for k, (source, target) in enumerate(
            [(factor_hbm, factor_ref), (matrix_hbm, matrix_ref), (grad_hbm, grad_ref)]
        )
    ]
    for arrival in arrivals:
        arrival.start()
    width = matrix_ref.shape[1]
    count = width // BLOCK
    rows = BLOCK // CHUNKS
    row, col = row_col((BLOCK, BLOCK))
    on_diag = row == col
    lower, upper = lower_blocks(width), upper_blocks(width)
    upper_at, low_at, _ = pieces_of(width)

    def block_of(piece):
        return jnp.concatenate([packed_ref[c, piece] for c in range(CHUNKS)], axis=0)

    def trace_of(ref):
        total = jnp.zeros((1, 1), f32)
        for b in range(count):
            total += jnp.sum(jnp.where(on_diag, ref[span(b), span(b)], 0.0), keepdims=True)
        return total

    def shifted(block, shift):
        return block + jnp.where(on_diag, jnp.broadcast_to(shift, block.shape), 0.0)

    for place, (i, j) in enumerate(lower):
        block = block_of(place)
        if i == j:
            corner = packed_ref[0, low_at + place]
            diag = jnp.where(col[:1] == 0, corner[1:2, BLOCK - 1 :], corner[:1, :])
            diag = jnp.broadcast_to(diag, block.shape)
            cross_ref[span(i), span(i)] = jnp.where(row < col, block, jnp.where(on_diag, diag, 0.0))
            block = mirror_lower(block)
        else:
            cross_ref[span(i), span(j)] = jnp.zeros_like(block)
        sym_ref[span(i), span(j)] = block
    for place, (i, j) in enumerate(upper):
        cross_ref[span(i), span(j)] = block_of(upper_at + place)
    shift1 = trace_of(sym_ref) * rate
    for b in range(count):
        sym_ref[span(b), span(b)] = shifted(sym_ref[span(b), span(b)], shift1)
    cholesky_inverse(sym_ref, lower1_ref, inv1_ref, work_ref, tile_ref, corner_ref, unit_ref)

    for j, terms in enumerate(exact_terms(lower1_ref[...], True)):
        for i in range(j, count):
            place = lower.index((i, j))
            here = slice((i - j) * BLOCK, (i - j + 1) * BLOCK)
            high = block_of(place)
            rest = block_of(low_at + place)
            if i == j:
                high, error = two_sum(high, jnp.where(on_diag, jnp.broadcast_to(shift1, high.shape), 0.0))
                rest = rest + error
            high, error = two_sum(high, -terms[0][here])
            high, error2 = two_sum(high, -terms[1][here])
            rest = rest + (error + error2)
            for term in terms[2:]:
                rest = rest - term[here]
            block = high + rest
            if i == j:
                block = mirror_lower(block)
            else:
                full_ref[span(j), span(i)] = block.T
            full_ref[span(i), span(j)] = block
    inv1 = inv1_ref[...]
    spread = dot3(inv1, full_ref[...])
    for arrival in arrivals:
        arrival.wait()
    early_ref[...] = upper_times_lower(factor_ref[...], lower1_ref[...])
    before_ref[...] = dot3(matrix_ref[...], inv1, 1, 1)
    cross_ref[...] = dot3(inv1, cross_ref[...])
    for j in range(count):
        lo = j * BLOCK
        hi = lo + BLOCK
        spread_ref[lo:, span(j)] = dot_nt(inv1[lo:, :hi], inv1[span(j), :hi])
        column = dot3(spread[lo:, :hi], inv1[span(j), :hi], 1, 1)
        column -= jnp.broadcast_to(shift1, (width - lo, BLOCK)) * spread_ref[lo:, span(j)]
        for i in range(j, count):
            block = column[(i - j) * BLOCK : (i - j + 1) * BLOCK]
            if i == j:
                block = mirror_lower(jnp.where(on_diag, block + 1.0, block))
            else:
                full_ref[span(j), span(i)] = block.T
            full_ref[span(i), span(j)] = block
    shift2 = trace_of(full_ref) * rate
    for i, j in lower:
        block = full_ref[span(i), span(j)]
        sym_ref[span(i), span(j)] = shifted(block, shift2) if i == j else block
    cholesky_inverse(sym_ref, lower2_ref, inv2_ref, work_ref, tile_ref, corner_ref, unit_ref)

    inv1, inv2, lower1, lower2 = inv1_ref[...], inv2_ref[...], lower1_ref[...], lower2_ref[...]
    wide_row, wide_col = row_col((width, width))
    half = times_lower(cross_ref[...], inv2)
    second = early_ref[...] - lower_times_upper(inv2, half)
    middle = 0.5 * mirror_upper(upper_times_lower(second, lower2))
    side = times_lower(middle, inv2)
    weight = dot3(inv2, side, 0, 0) + jnp.where(wide_row == wide_col, rate * jnp.sum(side * inv2, keepdims=True), 0.0)
    crossed = half + 2.0 * dot3(full_ref[...], weight)
    first = lower_times_upper(lower2, factor_ref[...]) - upper_times_lower(crossed, inv1)
    middle = 0.5 * mirror_upper(upper_times_lower(first, lower1))
    trace = jnp.zeros((1, 1), f32)
    for i, j in lower:
        part = jnp.sum(middle[span(i), span(j)] * spread_ref[span(i), span(j)], keepdims=True)
        trace += part if i == j else 2.0 * part
    through = dot3(grad_ref[...], inv2) + 2.0 * dot3(before_ref[...], weight + middle)
    out_ref[...] = dot3(through, inv1) + (2.0 * rate) * trace * matrix_ref[...]


def exchange_levels(count):
    levels, stride = [], 1
    while stride < count:
        left = count // stride
        size = left if left <= 8 and levels else min(4, left)
        levels.append((stride, size))
        stride *= size
    return levels


def sum_over_devices(value, counts, low):
    rows_count, sub_count = counts
    levels = [("sub", 1, sub_count)] + [("rows", s, n) for s, n in exchange_levels(rows_count)]
    totals = {"rows": rows_count, "sub": sub_count}
    many, start = low

    def send(array, axis, change):
        return lax.ppermute(array, axis, [(i, i ^ change) for i in range(totals[axis])])

    def swap(mine, axis, stride):
        mine = lax.optimization_barrier(tuple(mine))
        return lax.optimization_barrier(
            (mine[0],) + tuple(send(mine[k], axis, k * stride) for k in range(1, len(mine)))
        )

    def add(left, right):
        total, error = two_sum(left, right)
        pad = [(0, 0)] * (total.ndim - 3) + [(start, 0), (0, 0), (0, 0)]
        return total + jnp.pad(error[..., :many, :, :], pad)

    def tree(values):
        while len(values) > 1:
            values = [add(values[i], values[i + 1]) for i in range(0, len(values), 2)]
        return values[0]

    split = []
    for axis, stride, size in levels:
        if value.shape[0] % size == 0:
            spot = (lax.axis_index(axis) // stride) % size
            pieces = value.reshape((size, value.shape[0] // size) + value.shape[1:])
            mine = [lax.dynamic_index_in_dim(pieces, spot ^ other, 0, False) for other in range(size)]
            split.append((axis, stride, size, spot))
            value = tree(swap(mine, axis, stride))
        else:
            change = 1
            while change < size:
                value = add(value, send(value, axis, change * stride))
                change = 2 * change + 1
    for axis, stride, size, spot in split[::-1]:
        got = swap([value] * size, axis, stride)
        pieces = jnp.zeros((size,) + value.shape, f32)
        for other in range(size):
            pieces = lax.dynamic_update_index_in_dim(pieces, got[other], spot ^ other, 0)
        value = pieces.reshape((size * value.shape[0],) + value.shape[1:])
    return value


def call(kernel, out_shapes, scratch_shapes, *operands, spaces=None):
    vmem = pl.BlockSpec(memory_space=pltpu.VMEM)
    return pl.pallas_call(
        kernel,
        out_shape=out_shapes,
        in_specs=spaces or [vmem] * len(operands),
        out_specs=[vmem] * len(out_shapes),
        scratch_shapes=scratch_shapes,
    )(*operands)


def run_gram(matrix, grad_out):
    shape = (CHUNKS, pieces_of(matrix.shape[1])[2], BLOCK // CHUNKS, BLOCK)
    return call(gram_kernel, [pltpu.VMEM(shape, f32)], [], matrix, grad_out)[0]


def run_main(packed, grad_factor, matrix, grad_out):
    width = matrix.shape[1]
    square, tile, rows = [pltpu.VMEM(s, f32) for s in ((width, width), (BLOCK, BLOCK), matrix.shape)]

    def main(*refs):
        main_kernel(*refs, rate=shift_frac / width)

    packed = pltpu.with_memory_space_constraint(packed, pltpu.VMEM)
    scratch = [square] * 10 + [tile] * 4 + [rows] * 3 + [pltpu.SemaphoreType.DMA((3,))]
    spaces = [pl.BlockSpec(memory_space=pltpu.VMEM)] + [pl.BlockSpec(memory_space=pl.ANY)] * 3
    out = jax.ShapeDtypeStruct(matrix.shape, f32)
    return call(main, [out], scratch, packed, grad_factor, matrix, grad_out, spaces=spaces)[0]


def solution(mesh):
    counts = (mesh.shape["rows"], mesh.shape["sub"])

    def per_device(matrix, grad_out, grad_factor):
        many, start, _ = pieces_of(matrix.shape[1])
        packed = sum_over_devices(run_gram(matrix, grad_out), counts, (many, start))
        return run_main(packed, grad_factor, matrix, grad_out)

    placed = (P(("rows", "sub"), None), P(("rows", "sub"), None), P())
    return jax.shard_map(
        per_device, mesh=mesh, in_specs=placed, out_specs=P(("rows", "sub"), None), check_vma=False
    )
```
